128 devices in a mesh: tree: 1, feat: 16 (over z, y), data: 8 (over x, core).
Axes of the slice: x: 4, y: 4, z: 4, core: 2. Of those that a mesh axis runs over, the one named last changes fastest.
Arguments:
- binned: int32 [4096, 128], P(('tree', 'data'), 'feat')
- gradient: float32 [4096], P(('tree', 'data'))
- hessian: float32 [4096], P(('tree', 'data'))
- split_feat: int32 [7, 64], P('tree')
- split_thr: int32 [7, 64], P('tree')
- reg_lambda: float32 [1], replicated
Outputs:
- output 1: float32 [255, 128, 255], P('tree', ('feat', 'data'))
- output 2: float32 [128], P('tree')
All inputs are finite; a program needn't handle non-finite values.
Results may differ from the reference program's by a relative error of at most 0.001.
Values sent between devices are 32-bit elements.
A program may use at most 1 GiB of HBM per device.

```python
import jax
import jax.numpy as jnp
from jax import lax

ROWS = 4096
FEATS = 128
NBINS = 256
DEPTH = 8
LEAVES = 2 ** (DEPTH - 1)
WIDTH = 2 ** (DEPTH - 2)
LAM_SCALE = max(1, ROWS // (LEAVES * NBINS))


def setup_inputs(seed: int = 0, part: int = 0) -> dict:
    base_key = jax.random.key(seed)
    part_key = jax.random.fold_in(base_key, part)
    key_bins, key_grad, key_hess, key_feat, key_thr = jax.random.split(part_key, 5)
    binned = jax.random.randint(key_bins, (ROWS, FEATS), 0, NBINS, dtype=jnp.int32)
    gradient = 0.25 + jax.random.normal(key_grad, (ROWS,), jnp.float32)
    hessian = jax.random.uniform(key_hess, (ROWS,), jnp.float32, 0.1, 1.9)
    split_feat = jax.random.randint(key_feat, (DEPTH - 1, WIDTH), 0, FEATS, dtype=jnp.int32)
    split_thr = jax.random.randint(key_thr, (DEPTH - 1, WIDTH), NBINS // 8, NBINS - NBINS // 8, dtype=jnp.int32)
    reg_lambda = LAM_SCALE * jax.random.uniform(jax.random.key(seed + 1), (1,), jnp.float32, 0.5, 2.0)
    return {'binned': binned, 'gradient': gradient, 'hessian': hessian, 'split_feat': split_feat, 'split_thr': split_thr, 'reg_lambda': reg_lambda}


def level_histogram(columns, node, grad_hess, n_nodes):
    def one_feature(column):
        return jax.ops.segment_sum(grad_hess, node * NBINS + column, num_segments=n_nodes * NBINS)
    histogram = lax.map(one_feature, columns)
    return histogram.reshape(FEATS, n_nodes, NBINS, 2)


def node_score(pair_sums, reg_value):
    return pair_sums[..., 0] ** 2 / (pair_sums[..., 1] + reg_value)


def reference(binned, gradient, hessian, split_feat, split_thr, reg_lambda):
    reg_value = reg_lambda[0]
    grad_hess = jnp.stack([gradient, hessian], axis=1)
    columns = binned.T
    node = jnp.zeros((ROWS,), jnp.int32)
    pieces = []
    for level in range(DEPTH):
        histogram = level_histogram(columns, node, grad_hess, 2 ** level)
        left_sum = jnp.cumsum(histogram, axis=2)[:, :, :-1]
        node_sum = jnp.sum(histogram, axis=2, keepdims=True)
        gain = 0.5 * (node_score(left_sum, reg_value) + node_score(node_sum - left_sum, reg_value) - node_score(node_sum, reg_value))
        pieces.append(jnp.transpose(gain, (1, 0, 2)))
        if level < DEPTH - 1:
            chosen = split_feat[level][node]
            picked = jnp.take_along_axis(binned, chosen[:, None], axis=1)[:, 0]
            node = 2 * node + (picked > split_thr[level][node]).astype(jnp.int32)
    totals = jax.ops.segment_sum(grad_hess, node, num_segments=LEAVES)
    leaf_value = -totals[:, 0] / (totals[:, 1] + reg_value)
    return jnp.concatenate(pieces, axis=0), leaf_value
```

```python
import functools

import jax
import jax.numpy as jnp
from jax import lax
from jax.experimental import pallas as pl
from jax.experimental.pallas import tpu as pltpu
from jax.sharding import PartitionSpec as P

NBINS = 256
SIDE = 4
NF = SIDE * SIDE
ND = 8
CHUNK = 512
LEAVES = 128
MESH = pl.DeviceIdType.MESH


def split3(value):
    first = value.astype(jnp.bfloat16)
    rest = value - first.astype(jnp.float32)
    second = rest.astype(jnp.bfloat16)
    third = (rest - second.astype(jnp.float32)).astype(jnp.bfloat16)
    return first, second, third


def iota(shape, dim):
    return lax.broadcasted_iota(jnp.int32, shape, dim)


def contract_lanes(left, right):
    return lax.dot_general(left, right, (((1,), (1,)), ((), ())), preferred_element_type=jnp.float32)


def node_tables(feat_tbl, thr_tbl):
    lane = iota((8, 128), 1)
    feat_row = jnp.zeros((1, 128), jnp.int32)
    thr_row = jnp.zeros((1, 128), jnp.int32)
    for level in range(7):
        here = (lane >= 2 ** level) & (lane < 2 ** (level + 1))
        feat_row = feat_row + jnp.where(here, pltpu.roll(feat_tbl, 2 ** level, 1), 0)[level:level + 1]
        thr_row = thr_row + jnp.where(here, pltpu.roll(thr_tbl, 2 ** level, 1), 0)[level:level + 1]
    one, zero = jnp.float32(1), jnp.float32(0)
    by_feat = jnp.where(feat_row == iota((128, 128), 0), one, zero).astype(jnp.bfloat16)
    by_thr = jnp.broadcast_to(thr_row.astype(jnp.float32), (128, 128)).astype(jnp.bfloat16)
    position = iota((128, 128), 0)
    reverse = jnp.zeros((128, 128), jnp.int32)
    for bit in range(7):
        reverse = reverse | (((position >> bit) & 1) << (6 - bit))
    heap = jnp.zeros((128, 128), jnp.int32)
    for level in range(7):
        heap = jnp.where(position >= 2 ** level, 2 ** level + (reverse >> (7 - level)), heap)
    order = jnp.where(heap == iota((128, 128), 1), one, zero).astype(jnp.bfloat16)
    return contract_lanes(order, by_feat).astype(jnp.bfloat16), contract_lanes(order, by_thr)


def route(values, select, threshold):
    picked = jnp.dot(select, values, preferred_element_type=jnp.float32)
    limit = jnp.concatenate([threshold] * (values.shape[1] // 128), axis=1)
    right = picked > limit
    leaf = jnp.where(right[64:128], 1, 0)
    for level in range(5, -1, -1):
        n = 2 ** level
        leaf = jnp.where(right[n:2 * n], leaf[n:] + 2 ** (6 - level), leaf[:n])
    return leaf


def exchange_kernel(bin_hbm, grad_hbm, hess_hbm, feat_hbm, thr_hbm,
                    cols, grads, hesses, leaves,
                    values, feat_in, thr_in, feat_tbl, thr_tbl, local_sem,
                    feat_send, feat_recv, data_send, data_recv, leaf_send, leaf_recv):
    f, d = lax.axis_index('feat'), lax.axis_index('data')
    z, y = f // SIDE, f % SIDE
    shifts = [(a, b) for a in range(SIDE) for b in range(SIDE) if a or b]
    distance = lambda s: min(s[0], SIDE - s[0]) + min(s[1], SIDE - s[1])
    shifts.sort(key=lambda s: -distance(s))
    feat_peers = [((z + a) % SIDE) * SIDE + (y + b) % SIDE for a, b in shifts]
    data_peers = [(d + k) % ND for k in range(1, ND)]

    local = [
        pltpu.make_async_copy(bin_hbm, values.at[f], local_sem.at[0]),
        pltpu.make_async_copy(bin_hbm, cols.at[d], local_sem.at[1]),
        pltpu.make_async_copy(grad_hbm, grads.at[d], local_sem.at[2]),
        pltpu.make_async_copy(hess_hbm, hesses.at[d], local_sem.at[3]),
        pltpu.make_async_copy(feat_hbm, feat_in, local_sem.at[4]),
        pltpu.make_async_copy(thr_hbm, thr_in, local_sem.at[5]),
    ]
    barrier = pltpu.get_barrier_semaphore()
    for peer in feat_peers:
        pl.semaphore_signal(barrier, inc=1, device_id={'feat': peer}, device_id_type=MESH)
    for peer in data_peers:
        pl.semaphore_signal(barrier, inc=1, device_id={'data': peer}, device_id_type=MESH)
    for copy in local:
        copy.start()
    for copy in local:
        copy.wait()
    pl.semaphore_wait(barrier, NF - 1 + ND - 1)

    feat_copies = []
    for k, peer in enumerate(feat_peers):
        copy = pltpu.make_async_remote_copy(
            src_ref=values.at[f], dst_ref=values.at[f], send_sem=feat_send.at[k], recv_sem=feat_recv.at[k],
            device_id={'feat': peer}, device_id_type=MESH)
        copy.start()
        feat_copies.append(copy)
    data_copies = []
    for k, peer in enumerate(data_peers):
        for part, ref in enumerate((cols, grads, hesses)):
            copy = pltpu.make_async_remote_copy(
                src_ref=ref.at[d], dst_ref=ref.at[d], send_sem=data_send.at[part, k], recv_sem=data_recv.at[part, k],
                device_id={'data': peer}, device_id_type=MESH)
            copy.start()
            data_copies.append(copy)

    feat_tbl[...] = jnp.zeros_like(feat_tbl)
    thr_tbl[...] = jnp.zeros_like(thr_tbl)
    feat_tbl[0:7, 0:64] = feat_in[...]
    thr_tbl[0:7, 0:64] = thr_in[...]
    select, threshold = node_tables(feat_tbl[...], thr_tbl[...])
    for copy in feat_copies:
        copy.wait_recv()
    table = values[...].reshape(NF * 8, CHUNK).astype(jnp.float32).astype(jnp.bfloat16)
    leaves[d] = route(table, select, threshold)
    leaf_copies = []
    for k, peer in enumerate(data_peers):
        copy = pltpu.make_async_remote_copy(
            src_ref=leaves.at[d], dst_ref=leaves.at[d], send_sem=leaf_send.at[k], recv_sem=leaf_recv.at[k],
            device_id={'data': peer}, device_id_type=MESH)
        copy.start()
        leaf_copies.append(copy)
    for copy in feat_copies:
        copy.wait_send()
    for copy in data_copies + leaf_copies:
        copy.wait()


def gain_kernel(reg_ref, cols, grads, hesses, leaves, gain_ref, leaf_ref, heap_g, heap_h):
    mine = lax.axis_index('data')
    reg = reg_ref[0]
    zero = jnp.float32(0)
    total = jnp.zeros((2 * LEAVES, NBINS), jnp.float32)
    for d in range(ND):
        column = cols[d, pl.ds(mine, 1), :]
        below = jnp.where(column <= iota((NBINS, CHUNK), 0), jnp.float32(1), zero).astype(jnp.bfloat16)
        member = leaves[d] == iota((LEAVES, CHUNK), 0)
        for g, h in zip(split3(grads[d]), split3(hesses[d])):
            weights = jnp.concatenate([
                jnp.where(member, g.astype(jnp.float32), zero),
                jnp.where(member, h.astype(jnp.float32), zero)], axis=0).astype(jnp.bfloat16)
            total = total + contract_lanes(weights, below)
    for half in range(2):
        lanes = slice(128 * half, 128 * half + 128)
        heap_g[half, 128:256, :] = total[:LEAVES, lanes]
        heap_h[half, 128:256, :] = total[LEAVES:, lanes]
    for level in range(6, -1, -1):
        n = 2 ** level
        for half in range(2):
            for heap in (heap_g, heap_h):
                left = heap[half, pl.ds(2 * n, n, stride=2), :]
                right = heap[half, pl.ds(2 * n + 1, n, stride=2), :]
                heap[half, n:2 * n, :] = left + right

    def score(g, h):
        return g * g / (h + reg)

    for start in range(0, 255, 8):
        n = min(8, 255 - start)
        rows = pl.ds(1 + start, n)
        all_g = heap_g[1, rows, 127:128]
        all_h = heap_h[1, rows, 127:128]
        whole = score(all_g, all_h)
        for half in range(2):
            left_g, left_h = heap_g[half, rows, :], heap_h[half, rows, :]
            gain = 0.5 * (score(left_g, left_h) + score(all_g - left_g, all_h - left_h) - whole)
            wide = 128 - half
            gain_ref[pl.ds(start, n), 0, pl.ds(128 * half, wide)] = gain[:, :wide]
    value = -heap_g[1, 128:256, :] / (heap_h[1, 128:256, :] + reg)
    leaf_ref[...] = value.T[127:128, :]


def solution(mesh):
    def per_device(binned, gradient, hessian, split_feat, split_thr, reg_lambda):
        any_spec = pl.BlockSpec(memory_space=pl.ANY)
        vmem = pl.BlockSpec(memory_space=pltpu.VMEM)
        dma = pltpu.SemaphoreType.DMA
        cols, grads, hesses, leaves = pl.pallas_call(
            exchange_kernel,
            out_shape=[
                jax.ShapeDtypeStruct((ND, 8, CHUNK), jnp.int32),
                jax.ShapeDtypeStruct((ND, 1, CHUNK), jnp.float32),
                jax.ShapeDtypeStruct((ND, 1, CHUNK), jnp.float32),
                jax.ShapeDtypeStruct((ND, 1, CHUNK), jnp.int32),
            ],
            in_specs=[any_spec] * 5,
            out_specs=[vmem] * 4,
            scratch_shapes=[
                pltpu.VMEM((NF, 8, CHUNK), jnp.int32),
                pltpu.VMEM((7, 64), jnp.int32),
                pltpu.VMEM((7, 64), jnp.int32),
                pltpu.VMEM((8, 128), jnp.int32),
                pltpu.VMEM((8, 128), jnp.int32),
                dma((6,)),
                dma((NF - 1,)), dma((NF - 1,)),
                dma((3, ND - 1)), dma((3, ND - 1)),
                dma((ND - 1,)), dma((ND - 1,)),
            ],
            compiler_params=pltpu.CompilerParams(collective_id=0, has_side_effects=True),
            name='exchange',
        )(binned.T, gradient.reshape(1, CHUNK), hessian.reshape(1, CHUNK), split_feat, split_thr)
        gain, leaf_value = pl.pallas_call(
            gain_kernel,
            out_shape=[
                jax.ShapeDtypeStruct((255, 1, 255), jnp.float32),
                jax.ShapeDtypeStruct((1, LEAVES), jnp.float32),
            ],
            in_specs=[pl.BlockSpec(memory_space=pltpu.SMEM)] + [vmem] * 4,
            out_specs=[vmem] * 2,
            scratch_shapes=[pltpu.VMEM((2, 256, 128), jnp.float32), pltpu.VMEM((2, 256, 128), jnp.float32)],
            name='gains',
        )(reg_lambda, cols, grads, hesses, leaves)
        return gain, leaf_value.reshape(LEAVES)

    row_spec = P(('tree', 'data'))
    return jax.shard_map(
        per_device,
        mesh=mesh,
        in_specs=(P(('tree', 'data'), 'feat'), row_spec, row_spec, P('tree', None), P('tree', None), P(None)),
        out_specs=(P('tree', ('feat', 'data'), None), P('tree')),
        check_vma=False,
    )
```

```python
import jax
import jax.numpy as jnp
from jax import lax
from jax.experimental import pallas as pl
from jax.experimental.pallas import tpu as pltpu
from jax.sharding import PartitionSpec as P

NBINS = 256
SIDE = 4
NF = SIDE * SIDE
ND = 8
CHUNK = 512
LEAVES = 128
FEAT_ORDER = sorted(range(NF), key=lambda f: min(f // SIDE, SIDE - f // SIDE) + min(f % SIDE, SIDE - f % SIDE))
MESH = pl.DeviceIdType.MESH


def split3(value):
    first = value.astype(jnp.bfloat16)
    rest = value - first.astype(jnp.float32)
    second = rest.astype(jnp.bfloat16)
    third = (rest - second.astype(jnp.float32)).astype(jnp.bfloat16)
    return first, second, third


def iota(shape, dim):
    return lax.broadcasted_iota(jnp.int32, shape, dim)


def contract_lanes(left, right):
    return lax.dot_general(left, right, (((1,), (1,)), ((), ())), preferred_element_type=jnp.float32)


def node_tables(feat_tbl, thr_tbl):
    lane = iota((8, 128), 1)
    feat_row = jnp.zeros((1, 128), jnp.int32)
    thr_row = jnp.zeros((1, 128), jnp.int32)
    for level in range(7):
        here = (lane >= 2 ** level) & (lane < 2 ** (level + 1))
        feat_row = feat_row + jnp.where(here, pltpu.roll(feat_tbl, 2 ** level, 1), 0)[level:level + 1]
        thr_row = thr_row + jnp.where(here, pltpu.roll(thr_tbl, 2 ** level, 1), 0)[level:level + 1]
    one, zero = jnp.float32(1), jnp.float32(0)
    by_feat = jnp.where(feat_row == iota((128, 128), 0), one, zero).astype(jnp.bfloat16)
    by_thr = jnp.broadcast_to(thr_row.astype(jnp.float32), (128, 128)).astype(jnp.bfloat16)
    position = iota((128, 128), 0)
    reverse = jnp.zeros((128, 128), jnp.int32)
    for bit in range(7):
        reverse = reverse | (((position >> bit) & 1) << (6 - bit))
    heap = jnp.zeros((128, 128), jnp.int32)
    for level in range(7):
        heap = jnp.where(position >= 2 ** level, 2 ** level + (reverse >> (7 - level)), heap)
    order = jnp.where(heap == iota((128, 128), 1), one, zero).astype(jnp.bfloat16)
    return contract_lanes(order, by_feat).astype(jnp.bfloat16), contract_lanes(order, by_thr)


def route(values, select, threshold):
    picked = jnp.dot(select, values, preferred_element_type=jnp.float32)
    limit = jnp.concatenate([threshold] * (values.shape[1] // 128), axis=1)
    right = picked > limit
    leaf = jnp.where(right[64:128], 1, 0)
    for level in range(5, -1, -1):
        n = 2 ** level
        leaf = jnp.where(right[n:2 * n], leaf[n:] + 2 ** (6 - level), leaf[:n])
    return leaf


def exchange_kernel(bin_hbm, grad_hbm, hess_hbm, feat_hbm, thr_hbm, reg_hbm, sums, leaf_sums, reg_row,
                    values, parcels, rows, leaves, below, own_bins, own_grad, own_hess, reg_in, feat_in, thr_in, feat_tbl, thr_tbl,
                    local_sem, feat_send, feat_recv, data_send, data_recv, leaf_send, leaf_recv):
    f, d = lax.axis_index('feat'), lax.axis_index('data')
    x, core = d // 2, d % 2
    near = x + 1 - 2 * (x % 2)
    lines = [near, SIDE - 1 - x, (x + 2) % SIDE]
    data_peers = [2 * x + 1 - core] + [2 * line + c for c in (1, 0) for line in lines]

    own = pltpu.make_async_copy(bin_hbm, values.at[f], feat_recv)
    local = [
        pltpu.make_async_copy(bin_hbm, own_bins, local_sem.at[0]),
        pltpu.make_async_copy(grad_hbm, own_grad, local_sem.at[1]),
        pltpu.make_async_copy(hess_hbm, own_hess, local_sem.at[2]),
        pltpu.make_async_copy(feat_hbm, feat_in, local_sem.at[3]),
        pltpu.make_async_copy(thr_hbm, thr_in, local_sem.at[4]),
        pltpu.make_async_copy(reg_hbm, reg_in, local_sem.at[5]),
    ]
    barrier = pltpu.get_barrier_semaphore()
    own.start()
    for peer in FEAT_ORDER:
        @pl.when(peer != f)
        def _():
            pl.semaphore_signal(barrier, inc=1, device_id={'feat': peer}, device_id_type=MESH)
    for peer in data_peers:
        pl.semaphore_signal(barrier, inc=1, device_id={'data': peer}, device_id_type=MESH)
    for copy in local:
        copy.start()
    pl.semaphore_wait(barrier, NF - 1 + ND - 1)

    for peer in FEAT_ORDER:
        copy = pltpu.make_async_remote_copy(
            src_ref=bin_hbm, dst_ref=values.at[f], send_sem=feat_send, recv_sem=feat_recv,
            device_id={'feat': peer}, device_id_type=MESH)
        pl.when(peer != f)(copy.start)
    for copy in local:
        copy.wait()
    for peer in range(ND):
        parcels[peer, 0] = own_bins[peer:peer + 1, :].astype(jnp.float32)
        parcels[peer, 1] = own_grad[...]
        parcels[peer, 2] = own_hess[...]
    for peer in data_peers:
        pltpu.make_async_remote_copy(
            src_ref=parcels.at[peer], dst_ref=rows.at[d], send_sem=data_send, recv_sem=data_recv,
            device_id={'data': peer}, device_id_type=MESH).start()
    rows[d] = parcels[d]

    reg_row[...] = jnp.broadcast_to(reg_in[0], (1, 128))
    feat_tbl[...] = jnp.zeros_like(feat_tbl)
    thr_tbl[...] = jnp.zeros_like(thr_tbl)
    feat_tbl[0:7, 0:64] = feat_in[...]
    thr_tbl[0:7, 0:64] = thr_in[...]
    select, threshold = node_tables(feat_tbl[...], thr_tbl[...])
    pltpu.make_async_copy(values, values, feat_recv).wait()
    table = values[...].reshape(NF * 8, CHUNK).astype(jnp.float32).astype(jnp.bfloat16)
    leaves[d] = route(table, select, threshold)

    def leaf_copy(k):
        return pltpu.make_async_remote_copy(
            src_ref=leaves.at[d], dst_ref=leaves.at[d], send_sem=leaf_send, recv_sem=leaf_recv.at[d],
            device_id={'data': data_peers[k]}, device_id_type=MESH)
    for k in range(ND - 1):
        leaf_copy(k).start()

    zero = jnp.float32(0)
    arrived = rows.at[pl.ds(0, ND - 1)]
    pltpu.make_async_copy(arrived, arrived, data_recv).wait()
    sources = [d] + data_peers
    for k, s in enumerate(sources):
        below[k] = jnp.where(rows[s, 0].astype(jnp.int32) <= iota((NBINS, CHUNK), 0), jnp.float32(1), zero).astype(jnp.bfloat16)

    totals = [None, None]
    for k, s in enumerate(sources):
        if k:
            pltpu.make_async_copy(leaves.at[s], leaves.at[s], leaf_recv.at[s]).wait()
        member = leaves[s] == iota((LEAVES, CHUNK), 0)
        mark = jnp.where(member, jnp.float32(1), zero).astype(jnp.bfloat16)
        for part in range(2):
            value = rows[s, 1 + part]
            inside = jnp.where(member, value, zero)
            leaf_sums[s, part] = inside[:, :128] + inside[:, 128:256] + (inside[:, 256:384] + inside[:, 384:])
            product = contract_lanes(jnp.concatenate([mark * piece for piece in split3(value)], axis=0), below[k])
            product = product[:LEAVES] + product[LEAVES:2 * LEAVES] + product[2 * LEAVES:]
            totals[part] = product if k == 0 else totals[part] + product
    for part in range(2):
        for half in range(2):
            sums[part, half] = totals[part][:, 128 * half:128 * (half + 1)]
    sent = values.at[pl.ds(0, NF - 1)]
    pltpu.make_async_copy(sent, sent, feat_send).wait()
    pltpu.make_async_copy(arrived, arrived, data_send).wait()
    told = leaves.at[pl.ds(0, ND - 1)]
    pltpu.make_async_copy(told, told, leaf_send).wait()


def gain_kernel(reg_row, sums, leaf_sums, gain_hbm, leaf_hbm, heap, gains, leaf_row, out_sem):
    reg = reg_row[...]

    def score(g, h):
        return g * g / (h + reg)

    def fill(source, first, start, count):
        for r in range(start, start + count, 8):
            n = min(8, start + count - r)
            rows = pl.ds(r - first, n)
            all_g = source[0, 1, rows, 127:128]
            all_h = source[1, 1, rows, 127:128]
            whole = score(all_g, all_h)
            for half in range(2):
                left_g, left_h = source[0, half, rows, :], source[1, half, rows, :]
                gain = 0.5 * (score(left_g, left_h) + score(all_g - left_g, all_h - left_h) - whole)
                wide = 128 - half
                gains[pl.ds(r, n), 0, pl.ds(128 * half, wide)] = gain[:, :wide]
        send(gains.at[pl.ds(start, count)], gain_hbm.at[pl.ds(start, count)])

    copies = []

    def send(source, target):
        copy = pltpu.make_async_copy(source, target, out_sem.at[len(copies)])
        copy.start()
        copies.append(copy)

    leaf_total = []
    for part in range(2):
        whole = leaf_sums[0, part]
        for s in range(1, ND):
            whole = whole + leaf_sums[s, part]
        leaf_total.append(jnp.sum(whole.T, axis=0, keepdims=True))
    leaf_row[...] = -leaf_total[0] / (leaf_total[1] + reg)
    send(leaf_row, leaf_hbm)
    fill(sums, 127, 127, 64)
    fill(sums, 127, 191, 64)
    for level in range(6, -1, -1):
        n = 2 ** level
        source, base = (sums, 0) if level == 6 else (heap, 2 * n)
        for part in range(2):
            for half in range(2):
                heap[part, half, n:2 * n, :] = (source[part, half, pl.ds(base, n, stride=2), :]
                                                + source[part, half, pl.ds(base + 1, n, stride=2), :])
    fill(heap, -1, 0, 127)
    for copy in copies:
        copy.wait()


def solution(mesh):
    def per_device(binned, gradient, hessian, split_feat, split_thr, reg_lambda):
        hbm = pl.BlockSpec(memory_space=pltpu.HBM)
        vmem = pl.BlockSpec(memory_space=pltpu.VMEM)
        dma = pltpu.SemaphoreType.DMA
        inputs = [binned.T, gradient.reshape(1, CHUNK), hessian.reshape(1, CHUNK), split_feat, split_thr]
        sums, leaf_sums, reg_row = pl.pallas_call(
            exchange_kernel,
            out_shape=[
                jax.ShapeDtypeStruct((2, 2, LEAVES, 128), jnp.float32),
                jax.ShapeDtypeStruct((ND, 2, LEAVES, 128), jnp.float32),
                jax.ShapeDtypeStruct((1, 128), jnp.float32),
            ],
            in_specs=[hbm] * 5 + [pl.BlockSpec(memory_space=pl.ANY)],
            out_specs=[vmem] * 3,
            scratch_shapes=[
                pltpu.VMEM((NF, 8, CHUNK), jnp.int32),
                pltpu.VMEM((ND, 3, 1, CHUNK), jnp.float32),
                pltpu.VMEM((ND, 3, 1, CHUNK), jnp.float32),
                pltpu.VMEM((ND, 1, CHUNK), jnp.int32),
                pltpu.VMEM((ND, NBINS, CHUNK), jnp.bfloat16),
                pltpu.VMEM((8, CHUNK), jnp.int32),
                pltpu.VMEM((1, CHUNK), jnp.float32),
                pltpu.VMEM((1, CHUNK), jnp.float32),
                pltpu.SMEM((1,), jnp.float32),
                pltpu.VMEM((7, 64), jnp.int32),
                pltpu.VMEM((7, 64), jnp.int32),
                pltpu.VMEM((8, 128), jnp.int32),
                pltpu.VMEM((8, 128), jnp.int32),
                dma((6,)), dma, dma, dma, dma, dma, dma((ND,)),
            ],
            compiler_params=pltpu.CompilerParams(collective_id=0, has_side_effects=True, vmem_limit_bytes=24 * 2 ** 20),
            name='exchange',
        )(*[pltpu.with_memory_space_constraint(a, pltpu.HBM) for a in inputs], reg_lambda)
        gain, leaf_value = pl.pallas_call(
            gain_kernel,
            out_shape=[
                jax.ShapeDtypeStruct((255, 1, 255), jnp.float32),
                jax.ShapeDtypeStruct((1, LEAVES), jnp.float32),
            ],
            in_specs=[vmem] * 3,
            out_specs=[hbm] * 2,
            scratch_shapes=[
                pltpu.VMEM((2, 2, LEAVES, 128), jnp.float32),
                pltpu.VMEM((255, 1, 255), jnp.float32),
                pltpu.VMEM((1, LEAVES), jnp.float32),
                dma((4,)),
            ],
            compiler_params=pltpu.CompilerParams(vmem_limit_bytes=24 * 2 ** 20),
            name='gains',
        )(reg_row, sums, leaf_sums)
        return gain, leaf_value.reshape(LEAVES)

    row_spec = P(('tree', 'data'))
    return jax.shard_map(
        per_device,
        mesh=mesh,
        in_specs=(P(('tree', 'data'), 'feat'), row_spec, row_spec, P('tree', None), P('tree', None), P(None)),
        out_specs=(P('tree', ('feat', 'data'), None), P('tree')),
        check_vma=False,
    )
```

```python
import jax
import jax.numpy as jnp
from jax import lax
from jax.experimental import pallas as pl
from jax.experimental.pallas import tpu as pltpu
from jax.sharding import PartitionSpec as P

NBINS = 256
SIDE = 4
NF = SIDE * SIDE
ND = 8
CHUNK = 512
LEAVES = 128
HUB = 1
FEAT_ORDER = (0, 1, 4, 2, 5, 3, 8, 6, 9, 7, 10, 11, 12, 13, 14, 15)
FEAT_RANK = [FEAT_ORDER.index(f) for f in range(NF)]
DATA_ORDER = (1, 0, 3, 2, 5, 4, 7, 6)
MESH = pl.DeviceIdType.MESH


def split3(value):
    first = value.astype(jnp.bfloat16)
    rest = value - first.astype(jnp.float32)
    second = rest.astype(jnp.bfloat16)
    third = (rest - second.astype(jnp.float32)).astype(jnp.bfloat16)
    return first, second, third


def iota(shape, dim):
    return lax.broadcasted_iota(jnp.int32, shape, dim)


def contract_lanes(left, right):
    return lax.dot_general(left, right, (((1,), (1,)), ((), ())), preferred_element_type=jnp.float32)


def node_tables(feat_tbl, thr_tbl):
    lane = iota((8, 128), 1)
    feat_row = jnp.zeros((1, 128), jnp.int32)
    thr_row = jnp.zeros((1, 128), jnp.int32)
    for level in range(7):
        here = (lane >= 2 ** level) & (lane < 2 ** (level + 1))
        feat_row = feat_row + jnp.where(here, pltpu.roll(feat_tbl, 2 ** level, 1), 0)[level:level + 1]
        thr_row = thr_row + jnp.where(here, pltpu.roll(thr_tbl, 2 ** level, 1), 0)[level:level + 1]
    one, zero = jnp.float32(1), jnp.float32(0)
    by_feat = jnp.where(feat_row == iota((128, 128), 0), one, zero).astype(jnp.bfloat16)
    by_thr = jnp.broadcast_to(thr_row.astype(jnp.float32), (128, 128)).astype(jnp.bfloat16)
    position = iota((128, 128), 0)
    reverse = jnp.zeros((128, 128), jnp.int32)
    for bit in range(7):
        reverse = reverse | (((position >> bit) & 1) << (6 - bit))
    heap = jnp.zeros((128, 128), jnp.int32)
    for level in range(7):
        heap = jnp.where(position >= 2 ** level, 2 ** level + (reverse >> (7 - level)), heap)
    order = jnp.where(heap == iota((128, 128), 1), one, zero).astype(jnp.bfloat16)
    return contract_lanes(order, by_feat).astype(jnp.bfloat16), contract_lanes(order, by_thr)


def route(values, select, threshold):
    picked = jnp.dot(select, values, preferred_element_type=jnp.float32)
    limit = jnp.concatenate([threshold] * (values.shape[1] // 128), axis=1)
    right = picked > limit
    leaf = jnp.where(right[64:128], 1, 0)
    for level in range(5, -1, -1):
        n = 2 ** level
        leaf = jnp.where(right[n:2 * n], leaf[n:] + 2 ** (6 - level), leaf[:n])
    return leaf


def exchange_kernel(bin_hbm, grad_hbm, hess_hbm, feat_hbm, thr_hbm, reg_hbm, sums, leaf_sums, reg_row,
                    values, parcels, rows, leaves, below, own_bins, own_grad, own_hess, reg_in, feat_in, thr_in, feat_tbl, thr_tbl,
                    local_sem, ready, gathered, everyone, earlier_ok, later_ok,
                    block_send, block_recv, data_send, data_recv, leaf_send, leaf_recv):
    f, d = lax.axis_index('feat'), lax.axis_index('data')
    x, core = d // 2, d % 2
    chief, other = 2 * x + 1, 2 * x + 1 - core
    near = x + 1 - 2 * (x % 2)
    lines = [near, (x + 2) % SIDE, SIDE - 1 - x]
    data_peers = [other] + [2 * line + c for c in (1, 0) for line in lines]
    rank = sum(jnp.where(f == peer, FEAT_RANK[peer], 0) for peer in range(NF))
    is_chief = core == 1

    own = pltpu.make_async_copy(bin_hbm, values.at[1, f], block_recv.at[1])
    local = [
        pltpu.make_async_copy(bin_hbm, own_bins, local_sem.at[0]),
        pltpu.make_async_copy(grad_hbm, own_grad, local_sem.at[1]),
        pltpu.make_async_copy(hess_hbm, own_hess, local_sem.at[2]),
        pltpu.make_async_copy(feat_hbm, feat_in, local_sem.at[3]),
        pltpu.make_async_copy(thr_hbm, thr_in, local_sem.at[4]),
        pltpu.make_async_copy(reg_hbm, reg_in, local_sem.at[5]),
    ]
    barrier = pltpu.get_barrier_semaphore()

    def signal(semaphore, **device):
        pl.semaphore_signal(semaphore, inc=1, device_id=device, device_id_type=MESH)

    def send_block(peer, group):
        pltpu.make_async_remote_copy(
            src_ref=bin_hbm, dst_ref=values.at[group, f], send_sem=block_send, recv_sem=block_recv.at[group],
            device_id={'feat': peer, 'data': chief}, device_id_type=MESH).start()

    @pl.when(is_chief)
    def _():
        for peer in reversed(FEAT_ORDER):
            pl.when(FEAT_RANK[peer] > rank)(lambda: signal(barrier, feat=peer))
        signal(barrier, data=other)

        @pl.when(d == HUB)
        def _():
            for peer in data_peers:
                signal(barrier, data=peer)
        own.start()
    pl.when(jnp.logical_not(is_chief))(lambda: signal(barrier, data=other))
    for copy in local:
        copy.start()

    @pl.when(is_chief)
    def _():
        pl.semaphore_wait(barrier, rank + 1 + jnp.where(d == HUB, 0, 1))
        signal(earlier_ok, data=other)
        for peer in FEAT_ORDER:
            pl.when(FEAT_RANK[peer] < rank)(lambda: send_block(peer, 1))
        for peer in FEAT_ORDER:
            pl.when(FEAT_RANK[peer] < rank)(lambda: signal(ready, feat=peer))
        pl.when(d != HUB)(lambda: signal(gathered, data=HUB))

    @pl.when(jnp.logical_not(is_chief))
    def _():
        pl.semaphore_wait(barrier, 2)
        signal(gathered, data=HUB)
        pl.semaphore_wait(earlier_ok, 1)
        for peer in FEAT_ORDER:
            pl.when(FEAT_RANK[peer] <= rank)(lambda: send_block(peer, 0))

    for copy in local:
        copy.wait()
    for peer in range(ND):
        parcels[peer, 0] = own_bins[peer:peer + 1, :].astype(jnp.float32)
        parcels[peer, 1] = own_grad[...]
        parcels[peer, 2] = own_hess[...]
    rows[d] = parcels[d]

    @pl.when(d == HUB)
    def _():
        pl.semaphore_wait(gathered, ND - 1)
        for peer in data_peers:
            signal(everyone, data=peer)

    @pl.when(d != HUB)
    def _():
        pl.semaphore_wait(everyone, 1)
    for peer in data_peers:
        pltpu.make_async_remote_copy(
            src_ref=parcels.at[peer], dst_ref=rows.at[d], send_sem=data_send, recv_sem=data_recv,
            device_id={'data': peer}, device_id_type=MESH).start()

    @pl.when(is_chief)
    def _():
        pl.when(rank < NF - 1)(lambda: pl.semaphore_wait(ready, NF - 1 - rank))
        signal(later_ok, data=other)
        for peer in FEAT_ORDER:
            pl.when(FEAT_RANK[peer] > rank)(lambda: send_block(peer, 1))

    @pl.when(jnp.logical_not(is_chief))
    def _():
        pl.semaphore_wait(later_ok, 1)
        for peer in FEAT_ORDER:
            pl.when(FEAT_RANK[peer] > rank)(lambda: send_block(peer, 0))

    reg_row[...] = jnp.broadcast_to(reg_in[0], (1, 128))
    zero = jnp.float32(0)
    arrived = rows.at[pl.ds(0, ND - 1)]
    pltpu.make_async_copy(arrived, arrived, data_recv).wait()
    sources = [chief, chief - 1] + data_peers[1:]
    for k, s in enumerate(sources):
        below[k] = jnp.where(rows[s, 0].astype(jnp.int32) <= iota((NBINS, CHUNK), 0), jnp.float32(1), zero).astype(jnp.bfloat16)

    @pl.when(is_chief)
    def _():
        feat_tbl[...] = jnp.zeros_like(feat_tbl)
        thr_tbl[...] = jnp.zeros_like(thr_tbl)
        feat_tbl[0:7, 0:64] = feat_in[...]
        thr_tbl[0:7, 0:64] = thr_in[...]
        select, threshold = node_tables(feat_tbl[...], thr_tbl[...])
        for group in (1, 0):
            block = values.at[group]
            pltpu.make_async_copy(block, block, block_recv.at[group]).wait()
            s = chief - 1 + group
            table = values[group].reshape(NF * 8, CHUNK).astype(jnp.float32).astype(jnp.bfloat16)
            leaves[s] = route(table, select, threshold)
            for peer in DATA_ORDER:
                @pl.when(peer != d)
                def _():
                    pltpu.make_async_remote_copy(
                        src_ref=leaves.at[s], dst_ref=leaves.at[s], send_sem=leaf_send, recv_sem=leaf_recv.at[s],
                        device_id={'data': peer}, device_id_type=MESH).start()

    totals = [None, None]
    for k, s in enumerate(sources):
        arrival = pltpu.make_async_copy(leaves.at[s], leaves.at[s], leaf_recv.at[s])
        if k < 2:
            pl.when(jnp.logical_not(is_chief))(arrival.wait)
        else:
            arrival.wait()
        member = leaves[s] == iota((LEAVES, CHUNK), 0)
        mark = jnp.where(member, jnp.float32(1), zero).astype(jnp.bfloat16)
        for part in range(2):
            value = rows[s, 1 + part]
            inside = jnp.where(member, value, zero)
            leaf_sums[s, part] = inside[:, :128] + inside[:, 128:256] + (inside[:, 256:384] + inside[:, 384:])
            product = contract_lanes(jnp.concatenate([mark * piece for piece in split3(value)], axis=0), below[k])
            product = product[:LEAVES] + product[LEAVES:2 * LEAVES] + product[2 * LEAVES:]
            totals[part] = product if k == 0 else totals[part] + product
    for part in range(2):
        for half in range(2):
            sums[part, half] = totals[part][:, 128 * half:128 * (half + 1)]

    @pl.when(is_chief)
    def _():
        sent = values.at[0, pl.ds(0, NF - 1)]
        pltpu.make_async_copy(sent, sent, block_send).wait()
        told = leaves.at[pl.ds(0, ND - 1)]
        pltpu.make_async_copy(told, told, leaf_send).wait()
        pltpu.make_async_copy(told, told, leaf_send).wait()

    @pl.when(jnp.logical_not(is_chief))
    def _():
        sent = values.at[0]
        pltpu.make_async_copy(sent, sent, block_send).wait()
    pltpu.make_async_copy(arrived, arrived, data_send).wait()


def gain_kernel(reg_row, sums, leaf_sums, gain_hbm, leaf_hbm, heap, gains, leaf_row, out_sem):
    reg = reg_row[...]

    def score(g, h):
        return g * g / (h + reg)

    def fill(source, first, start, count):
        for r in range(start, start + count, 8):
            n = min(8, start + count - r)
            rows = pl.ds(r - first, n)
            all_g = source[0, 1, rows, 127:128]
            all_h = source[1, 1, rows, 127:128]
            whole = score(all_g, all_h)
            for half in range(2):
                left_g, left_h = source[0, half, rows, :], source[1, half, rows, :]
                gain = 0.5 * (score(left_g, left_h) + score(all_g - left_g, all_h - left_h) - whole)
                wide = 128 - half
                gains[pl.ds(r, n), 0, pl.ds(128 * half, wide)] = gain[:, :wide]
        send(gains.at[pl.ds(start, count)], gain_hbm.at[pl.ds(start, count)])

    copies = []

    def send(source, target):
        copy = pltpu.make_async_copy(source, target, out_sem.at[len(copies)])
        copy.start()
        copies.append(copy)

    leaf_total = []
    for part in range(2):
        whole = leaf_sums[0, part]
        for s in range(1, ND):
            whole = whole + leaf_sums[s, part]
        leaf_total.append(jnp.sum(whole.T, axis=0, keepdims=True))
    leaf_row[...] = -leaf_total[0] / (leaf_total[1] + reg)
    send(leaf_row, leaf_hbm)
    fill(sums, 127, 127, 64)
    fill(sums, 127, 191, 64)
    for level in range(6, -1, -1):
        n = 2 ** level
        source, base = (sums, 0) if level == 6 else (heap, 2 * n)
        for part in range(2):
            for half in range(2):
                heap[part, half, n:2 * n, :] = (source[part, half, pl.ds(base, n, stride=2), :]
                                                + source[part, half, pl.ds(base + 1, n, stride=2), :])
    fill(heap, -1, 0, 127)
    for copy in copies:
        copy.wait()


def solution(mesh):
    def per_device(binned, gradient, hessian, split_feat, split_thr, reg_lambda):
        hbm = pl.BlockSpec(memory_space=pltpu.HBM)
        vmem = pl.BlockSpec(memory_space=pltpu.VMEM)
        dma, regular = pltpu.SemaphoreType.DMA, pltpu.SemaphoreType.REGULAR
        inputs = [binned.T, gradient.reshape(1, CHUNK), hessian.reshape(1, CHUNK), split_feat, split_thr]
        sums, leaf_sums, reg_row = pl.pallas_call(
            exchange_kernel,
            out_shape=[
                jax.ShapeDtypeStruct((2, 2, LEAVES, 128), jnp.float32),
                jax.ShapeDtypeStruct((ND, 2, LEAVES, 128), jnp.float32),
                jax.ShapeDtypeStruct((1, 128), jnp.float32),
            ],
            in_specs=[hbm] * 5 + [pl.BlockSpec(memory_space=pl.ANY)],
            out_specs=[vmem] * 3,
            scratch_shapes=[
                pltpu.VMEM((2, NF, 8, CHUNK), jnp.int32),
                pltpu.VMEM((ND, 3, 1, CHUNK), jnp.float32),
                pltpu.VMEM((ND, 3, 1, CHUNK), jnp.float32),
                pltpu.VMEM((ND, 1, CHUNK), jnp.int32),
                pltpu.VMEM((ND, NBINS, CHUNK), jnp.bfloat16),
                pltpu.VMEM((8, CHUNK), jnp.int32),
                pltpu.VMEM((1, CHUNK), jnp.float32),
                pltpu.VMEM((1, CHUNK), jnp.float32),
                pltpu.SMEM((1,), jnp.float32),
                pltpu.VMEM((7, 64), jnp.int32),
                pltpu.VMEM((7, 64), jnp.int32),
                pltpu.VMEM((8, 128), jnp.int32),
                pltpu.VMEM((8, 128), jnp.int32),
                dma((6,)), regular, regular, regular, regular, regular,
                dma, dma((2,)), dma, dma, dma, dma((ND,)),
            ],
            compiler_params=pltpu.CompilerParams(collective_id=0, has_side_effects=True, vmem_limit_bytes=24 * 2 ** 20),
            name='exchange',
        )(*[pltpu.with_memory_space_constraint(a, pltpu.HBM) for a in inputs], reg_lambda)
        gain, leaf_value = pl.pallas_call(
            gain_kernel,
            out_shape=[
                jax.ShapeDtypeStruct((255, 1, 255), jnp.float32),
                jax.ShapeDtypeStruct((1, LEAVES), jnp.float32),
            ],
            in_specs=[vmem] * 3,
            out_specs=[hbm] * 2,
            scratch_shapes=[
                pltpu.VMEM((2, 2, LEAVES, 128), jnp.float32),
                pltpu.VMEM((255, 1, 255), jnp.float32),
                pltpu.VMEM((1, LEAVES), jnp.float32),
                dma((4,)),
            ],
            compiler_params=pltpu.CompilerParams(vmem_limit_bytes=24 * 2 ** 20),
            name='gains',
        )(reg_row, sums, leaf_sums)
        return gain, leaf_value.reshape(LEAVES)

    row_spec = P(('tree', 'data'))
    return jax.shard_map(
        per_device,
        mesh=mesh,
        in_specs=(P(('tree', 'data'), 'feat'), row_spec, row_spec, P('tree', None), P('tree', None), P(None)),
        out_specs=(P('tree', ('feat', 'data'), None), P('tree')),
        check_vma=False,
    )
```

```python
import jax
import jax.numpy as jnp
from jax import lax
from jax.experimental import pallas as pl
from jax.experimental.pallas import tpu as pltpu
from jax.sharding import PartitionSpec as P

NBINS = 256
SIDE = 4
NF = SIDE * SIDE
ND = 8
CHUNK = 512
LEAVES = 128
HUB = 0
FEAT_ORDER = (0, 1, 4, 2, 3, 5, 8, 10, 7, 9, 12, 6, 11, 14, 15, 13)
FEAT_RANK = [FEAT_ORDER.index(f) for f in range(NF)]
BUILD = {0: (0,), 1: (1,), 2: (2, 3), 3: (4, 5, 6, 7)}
DATA_ORDER = (1, 0, 3, 2, 5, 4, 7, 6)
MESH = pl.DeviceIdType.MESH


def split3(value):
    first = value.astype(jnp.bfloat16)
    rest = value - first.astype(jnp.float32)
    second = rest.astype(jnp.bfloat16)
    third = (rest - second.astype(jnp.float32)).astype(jnp.bfloat16)
    return first, second, third


def iota(shape, dim):
    return lax.broadcasted_iota(jnp.int32, shape, dim)


def contract_lanes(left, right):
    return lax.dot_general(left, right, (((1,), (1,)), ((), ())), preferred_element_type=jnp.float32)


def node_tables(feat_tbl, thr_tbl):
    lane = iota((8, 128), 1)
    feat_row = jnp.zeros((1, 128), jnp.int32)
    thr_row = jnp.zeros((1, 128), jnp.int32)
    for level in range(7):
        here = (lane >= 2 ** level) & (lane < 2 ** (level + 1))
        feat_row = feat_row + jnp.where(here, pltpu.roll(feat_tbl, 2 ** level, 1), 0)[level:level + 1]
        thr_row = thr_row + jnp.where(here, pltpu.roll(thr_tbl, 2 ** level, 1), 0)[level:level + 1]
    one, zero = jnp.float32(1), jnp.float32(0)
    by_feat = jnp.where(feat_row == iota((128, 128), 0), one, zero).astype(jnp.bfloat16)
    by_thr = jnp.broadcast_to(thr_row.astype(jnp.float32), (128, 128)).astype(jnp.bfloat16)
    position = iota((128, 128), 0)
    reverse = jnp.zeros((128, 128), jnp.int32)
    for bit in range(7):
        reverse = reverse | (((position >> bit) & 1) << (6 - bit))
    heap = jnp.zeros((128, 128), jnp.int32)
    for level in range(7):
        heap = jnp.where(position >= 2 ** level, 2 ** level + (reverse >> (7 - level)), heap)
    order = jnp.where(heap == iota((128, 128), 1), one, zero).astype(jnp.bfloat16)
    return contract_lanes(order, by_feat).astype(jnp.bfloat16), contract_lanes(order, by_thr)


def route(values, select, threshold):
    picked = jnp.dot(select, values, preferred_element_type=jnp.float32)
    limit = jnp.concatenate([threshold] * (values.shape[1] // 128), axis=1)
    right = picked > limit
    leaf = jnp.where(right[64:128], 1, 0)
    for level in range(5, -1, -1):
        n = 2 ** level
        leaf = jnp.where(right[n:2 * n], leaf[n:] + 2 ** (6 - level), leaf[:n])
    return leaf


def exchange_kernel(bin_hbm, grad_hbm, hess_hbm, feat_hbm, thr_hbm, reg_hbm, sums, leaf_row, reg_row,
                    leaf_sums, values, parcels, rows, columns, leaves, below, own_bins, own_grad, own_hess, reg_in, feat_in, thr_in, feat_tbl, thr_tbl,
                    local_sem, ready, gathered, everyone, earlier_ok, later_ok,
                    block_send, block_recv, data_send, data_recv, leaf_send, leaf_recv):
    f, d = lax.axis_index('feat'), lax.axis_index('data')
    x, core = d // 2, d % 2
    chief, other = 2 * x + 1, 2 * x + 1 - core
    near = x + 1 - 2 * (x % 2)
    lines = [near, (x + 2) % SIDE, SIDE - 1 - x]
    data_peers = [other] + [2 * line + c for c in (1, 0) for line in lines]
    rank = sum(jnp.where(f == peer, FEAT_RANK[peer], 0) for peer in range(NF))
    is_chief = core == 1

    own = pltpu.make_async_copy(bin_hbm, values.at[1, f], block_recv.at[1])
    local = [
        pltpu.make_async_copy(bin_hbm, own_bins, local_sem.at[0]),
        pltpu.make_async_copy(grad_hbm, own_grad, local_sem.at[1]),
        pltpu.make_async_copy(hess_hbm, own_hess, local_sem.at[2]),
        pltpu.make_async_copy(feat_hbm, feat_in, local_sem.at[3]),
        pltpu.make_async_copy(thr_hbm, thr_in, local_sem.at[4]),
        pltpu.make_async_copy(reg_hbm, reg_in, local_sem.at[5]),
    ]
    barrier = pltpu.get_barrier_semaphore()

    def signal(semaphore, **device):
        pl.semaphore_signal(semaphore, inc=1, device_id=device, device_id_type=MESH)

    def send_block(peer, group):
        pltpu.make_async_remote_copy(
            src_ref=bin_hbm, dst_ref=values.at[group, f], send_sem=block_send, recv_sem=block_recv.at[group],
            device_id={'feat': peer, 'data': chief}, device_id_type=MESH).start()

    @pl.when(is_chief)
    def _():
        for peer in reversed(FEAT_ORDER):
            pl.when(FEAT_RANK[peer] > rank)(lambda: signal(barrier, feat=peer))
        signal(barrier, data=other)
        own.start()

    @pl.when(jnp.logical_not(is_chief))
    def _():
        signal(barrier, data=other)

        @pl.when(d == HUB)
        def _():
            for peer in range(2, ND, 2):
                signal(barrier, data=peer)
    for copy in local:
        copy.start()

    @pl.when(is_chief)
    def _():
        pl.semaphore_wait(barrier, rank + 1)
        signal(earlier_ok, data=other)
        for peer in FEAT_ORDER:
            pl.when(FEAT_RANK[peer] < rank)(lambda: send_block(peer, 1))
        for peer in FEAT_ORDER:
            pl.when(FEAT_RANK[peer] < rank)(lambda: signal(ready, feat=peer))

    @pl.when(jnp.logical_not(is_chief))
    def _():
        pl.semaphore_wait(barrier, jnp.where(d == HUB, 1, 2))
        pl.when(d != HUB)(lambda: signal(gathered, data=HUB))
        pl.semaphore_wait(earlier_ok, 1)
        for peer in FEAT_ORDER:
            pl.when(FEAT_RANK[peer] <= rank)(lambda: send_block(peer, 0))

    for copy in local:
        copy.wait()
    for peer in range(ND):
        parcels[peer, 0] = own_bins[peer:peer + 1, :].astype(jnp.float32)
        parcels[peer, 1] = own_grad[...]
        parcels[peer, 2] = own_hess[...]
    rows[d] = parcels[d]

    @pl.when(d == HUB)
    def _():
        pl.semaphore_wait(gathered, SIDE - 1)
        for peer in data_peers:
            signal(everyone, data=peer)

    @pl.when(d != HUB)
    def _():
        pl.semaphore_wait(everyone, 1)
    for peer in data_peers:
        pltpu.make_async_remote_copy(
            src_ref=parcels.at[peer], dst_ref=rows.at[d], send_sem=data_send, recv_sem=data_recv,
            device_id={'data': peer}, device_id_type=MESH).start()

    @pl.when(is_chief)
    def _():
        pl.when(rank < NF - 1)(lambda: pl.semaphore_wait(ready, NF - 1 - rank))
        signal(later_ok, data=other)
        for peer in FEAT_ORDER:
            pl.when(FEAT_RANK[peer] > rank)(lambda: send_block(peer, 1))

    @pl.when(jnp.logical_not(is_chief))
    def _():
        pl.semaphore_wait(later_ok, 1)
        for peer in FEAT_ORDER:
            pl.when(FEAT_RANK[peer] > rank)(lambda: send_block(peer, 0))

    reg_row[...] = jnp.broadcast_to(reg_in[0], (1, 128))
    zero = jnp.float32(0)
    sources = [chief, chief - 1] + data_peers[1:]

    @pl.when(is_chief)
    def _():
        feat_tbl[...] = jnp.zeros_like(feat_tbl)
        thr_tbl[...] = jnp.zeros_like(thr_tbl)
        feat_tbl[0:7, 0:64] = feat_in[...]
        thr_tbl[0:7, 0:64] = thr_in[...]
        select, threshold = node_tables(feat_tbl[...], thr_tbl[...])
        for group in (1, 0):
            block = values.at[group]
            pltpu.make_async_copy(block, block, block_recv.at[group]).wait()
            s = chief - 1 + group
            table = values[group].reshape(NF * 8, CHUNK).astype(jnp.float32).astype(jnp.bfloat16)
            leaves[s] = route(table, select, threshold)
            for peer in DATA_ORDER:
                @pl.when(peer != d)
                def _():
                    pltpu.make_async_remote_copy(
                        src_ref=leaves.at[s], dst_ref=leaves.at[s], send_sem=leaf_send, recv_sem=leaf_recv.at[s],
                        device_id={'data': peer}, device_id_type=MESH).start()

    arrived = rows.at[pl.ds(0, ND - 1)]
    pltpu.make_async_copy(arrived, arrived, data_recv).wait()
    columns[...] = jnp.concatenate([rows[s, 0] for s in sources], axis=0).T

    def build(k):
        below[k] = jnp.where(columns[:, k:k + 1] <= iota((CHUNK, NBINS), 1).astype(jnp.float32), jnp.float32(1), zero).astype(jnp.bfloat16)

    totals = [None, None]
    for k, s in enumerate(sources):
        for later in BUILD.get(k, ()):
            build(later)
        arrival = pltpu.make_async_copy(leaves.at[s], leaves.at[s], leaf_recv.at[s])
        if k < 2:
            pl.when(jnp.logical_not(is_chief))(arrival.wait)
        else:
            arrival.wait()
        member = leaves[s] == iota((LEAVES, CHUNK), 0)
        mark = jnp.where(member, jnp.float32(1), zero).astype(jnp.bfloat16)
        for part in range(2):
            value = rows[s, 1 + part]
            inside = jnp.where(member, value, zero)
            leaf_sums[s, part] = inside[:, :128] + inside[:, 128:256] + (inside[:, 256:384] + inside[:, 384:])
            product = jnp.dot(jnp.concatenate([mark * piece for piece in split3(value)], axis=0), below[k], preferred_element_type=jnp.float32)
            product = product[:LEAVES] + product[LEAVES:2 * LEAVES] + product[2 * LEAVES:]
            totals[part] = product if k == 0 else totals[part] + product
    leaf_total = []
    for part in range(2):
        whole = leaf_sums[0, part]
        for s in range(1, ND):
            whole = whole + leaf_sums[s, part]
        leaf_total.append(jnp.sum(whole.T, axis=0, keepdims=True))
    leaf_row[...] = -leaf_total[0] / (leaf_total[1] + reg_row[...])
    for part in range(2):
        for half in range(2):
            sums[part, half] = totals[part][:, 128 * half:128 * (half + 1)]

    @pl.when(is_chief)
    def _():
        sent = values.at[0, pl.ds(0, NF - 1)]
        pltpu.make_async_copy(sent, sent, block_send).wait()
        told = leaves.at[pl.ds(0, ND - 1)]
        pltpu.make_async_copy(told, told, leaf_send).wait()
        pltpu.make_async_copy(told, told, leaf_send).wait()

    @pl.when(jnp.logical_not(is_chief))
    def _():
        sent = values.at[0]
        pltpu.make_async_copy(sent, sent, block_send).wait()
    pltpu.make_async_copy(arrived, arrived, data_send).wait()


def gain_kernel(reg_row, sums, leaf_row, gain_hbm, leaf_hbm, heap, gains, out_sem):
    reg = reg_row[...]

    def score(g, h):
        return g * g / (h + reg)

    def fill(source, first, start, count):
        for r in range(start, start + count, 8):
            n = min(8, start + count - r)
            rows = pl.ds(r - first, n)
            all_g = source[0, 1, rows, 127:128]
            all_h = source[1, 1, rows, 127:128]
            whole = score(all_g, all_h)
            for half in range(2):
                left_g, left_h = source[0, half, rows, :], source[1, half, rows, :]
                gain = 0.5 * (score(left_g, left_h) + score(all_g - left_g, all_h - left_h) - whole)
                wide = 128 - half
                gains[pl.ds(r, n), 0, pl.ds(128 * half, wide)] = gain[:, :wide]
        send(gains.at[pl.ds(start, count)], gain_hbm.at[pl.ds(start, count)])

    copies = []

    def send(source, target):
        copy = pltpu.make_async_copy(source, target, out_sem.at[len(copies)])
        copy.start()
        copies.append(copy)

    send(leaf_row, leaf_hbm)
    fill(sums, 127, 127, 64)
    fill(sums, 127, 191, 64)
    for level in range(6, -1, -1):
        n = 2 ** level
        source, base = (sums, 0) if level == 6 else (heap, 2 * n)
        for part in range(2):
            for half in range(2):
                heap[part, half, n:2 * n, :] = (source[part, half, pl.ds(base, n, stride=2), :]
                                                + source[part, half, pl.ds(base + 1, n, stride=2), :])
    fill(heap, -1, 0, 127)
    for copy in copies:
        copy.wait()


def solution(mesh):
    def per_device(binned, gradient, hessian, split_feat, split_thr, reg_lambda):
        hbm = pl.BlockSpec(memory_space=pltpu.HBM)
        vmem = pl.BlockSpec(memory_space=pltpu.VMEM)
        dma, regular = pltpu.SemaphoreType.DMA, pltpu.SemaphoreType.REGULAR
        inputs = [binned.T, gradient.reshape(1, CHUNK), hessian.reshape(1, CHUNK), split_feat, split_thr]
        sums, leaf_row, reg_row = pl.pallas_call(
            exchange_kernel,
            out_shape=[
                jax.ShapeDtypeStruct((2, 2, LEAVES, 128), jnp.float32),
                jax.ShapeDtypeStruct((1, LEAVES), jnp.float32),
                jax.ShapeDtypeStruct((1, 128), jnp.float32),
            ],
            in_specs=[hbm] * 5 + [pl.BlockSpec(memory_space=pl.ANY)],
            out_specs=[vmem] * 3,
            scratch_shapes=[
                pltpu.VMEM((ND, 2, LEAVES, 128), jnp.float32),
                pltpu.VMEM((2, NF, 8, CHUNK), jnp.int32),
                pltpu.VMEM((ND, 3, 1, CHUNK), jnp.float32),
                pltpu.VMEM((ND, 3, 1, CHUNK), jnp.float32),
                pltpu.VMEM((CHUNK, ND), jnp.float32),
                pltpu.VMEM((ND, 1, CHUNK), jnp.int32),
                pltpu.VMEM((ND, CHUNK, NBINS), jnp.bfloat16),
                pltpu.VMEM((8, CHUNK), jnp.int32),
                pltpu.VMEM((1, CHUNK), jnp.float32),
                pltpu.VMEM((1, CHUNK), jnp.float32),
                pltpu.SMEM((1,), jnp.float32),
                pltpu.VMEM((7, 64), jnp.int32),
                pltpu.VMEM((7, 64), jnp.int32),
                pltpu.VMEM((8, 128), jnp.int32),
                pltpu.VMEM((8, 128), jnp.int32),
                dma((6,)), regular, regular, regular, regular, regular,
                dma, dma((2,)), dma, dma, dma, dma((ND,)),
            ],
            compiler_params=pltpu.CompilerParams(collective_id=0, has_side_effects=True, vmem_limit_bytes=24 * 2 ** 20),
            name='exchange',
        )(*[pltpu.with_memory_space_constraint(a, pltpu.HBM) for a in inputs], reg_lambda)
        gain, leaf_value = pl.pallas_call(
            gain_kernel,
            out_shape=[
                jax.ShapeDtypeStruct((255, 1, 255), jnp.float32),
                jax.ShapeDtypeStruct((1, LEAVES), jnp.float32),
            ],
            in_specs=[vmem] * 3,
            out_specs=[hbm] * 2,
            scratch_shapes=[
                pltpu.VMEM((2, 2, LEAVES, 128), jnp.float32),
                pltpu.VMEM((255, 1, 255), jnp.float32),
                dma((4,)),
            ],
            compiler_params=pltpu.CompilerParams(vmem_limit_bytes=24 * 2 ** 20),
            name='gains',
        )(reg_row, sums, leaf_row)
        return gain, leaf_value.reshape(LEAVES)

    row_spec = P(('tree', 'data'))
    return jax.shard_map(
        per_device,
        mesh=mesh,
        in_specs=(P(('tree', 'data'), 'feat'), row_spec, row_spec, P('tree', None), P('tree', None), P(None)),
        out_specs=(P('tree', ('feat', 'data'), None), P('tree')),
        check_vma=False,
    )
```

```python
import jax
import jax.numpy as jnp
from jax import lax
from jax.experimental import pallas as pl
from jax.experimental.pallas import tpu as pltpu
from jax.sharding import PartitionSpec as P

NBINS = 256
SIDE = 4
NF = SIDE * SIDE
ND = 8
CHUNK = 512
LEAVES = 128
HUB = 0
FEAT_ORDER = (0, 1, 2, 4, 3, 8, 9, 7, 5, 12, 6, 10, 11, 14, 13, 15)
FEAT_RANK = [FEAT_ORDER.index(f) for f in range(NF)]
BUILD = {0: (0,), 1: (1,), 2: (2, 3), 3: (4, 5, 6, 7)}
SEND_ORDER = (0, 8, 15, 3, 2, 13, 4, 1, 5, 14, 7, 9, 11, 6, 12, 10)
RANK_GROUPS = ((0, 7), (8, 15))
DATA_ORDER = (1, 0, 3, 2, 5, 4, 7, 6)
MESH = pl.DeviceIdType.MESH


def split3(value):
    first = value.astype(jnp.bfloat16)
    rest = value - first.astype(jnp.float32)
    second = rest.astype(jnp.bfloat16)
    third = (rest - second.astype(jnp.float32)).astype(jnp.bfloat16)
    return first, second, third


def iota(shape, dim):
    return lax.broadcasted_iota(jnp.int32, shape, dim)


def contract_lanes(left, right):
    return lax.dot_general(left, right, (((1,), (1,)), ((), ())), preferred_element_type=jnp.float32)


def node_tables(feat_tbl, thr_tbl):
    lane = iota((8, 128), 1)
    feat_row = jnp.zeros((1, 128), jnp.int32)
    thr_row = jnp.zeros((1, 128), jnp.int32)
    for level in range(7):
        here = (lane >= 2 ** level) & (lane < 2 ** (level + 1))
        feat_row = feat_row + jnp.where(here, pltpu.roll(feat_tbl, 2 ** level, 1), 0)[level:level + 1]
        thr_row = thr_row + jnp.where(here, pltpu.roll(thr_tbl, 2 ** level, 1), 0)[level:level + 1]
    one, zero = jnp.float32(1), jnp.float32(0)
    by_feat = jnp.where(feat_row == iota((128, 128), 0), one, zero).astype(jnp.bfloat16)
    by_thr = jnp.broadcast_to(thr_row.astype(jnp.float32), (128, 128)).astype(jnp.bfloat16)
    position = iota((128, 128), 0)
    reverse = jnp.zeros((128, 128), jnp.int32)
    for bit in range(7):
        reverse = reverse | (((position >> bit) & 1) << (6 - bit))
    heap = jnp.zeros((128, 128), jnp.int32)
    for level in range(7):
        heap = jnp.where(position >= 2 ** level, 2 ** level + (reverse >> (7 - level)), heap)
    order = jnp.where(heap == iota((128, 128), 1), one, zero).astype(jnp.bfloat16)
    return contract_lanes(order, by_feat).astype(jnp.bfloat16), contract_lanes(order, by_thr)


def route(values, select, threshold):
    picked = jnp.dot(select, values, preferred_element_type=jnp.float32)
    limit = jnp.concatenate([threshold] * (values.shape[1] // 128), axis=1)
    right = picked > limit
    leaf = jnp.where(right[64:128], 1, 0)
    for level in range(5, -1, -1):
        n = 2 ** level
        leaf = jnp.where(right[n:2 * n], leaf[n:] + 2 ** (6 - level), leaf[:n])
    return leaf


def exchange_kernel(bin_hbm, grad_hbm, hess_hbm, feat_hbm, thr_hbm, reg_hbm, sums, leaf_row, reg_row,
                    leaf_sums, values, parcels, rows, columns, leaves, below, own_bins, own_grad, own_hess, reg_in, feat_in, thr_in, feat_tbl, thr_tbl,
                    local_sem, ready, gathered, everyone, earlier_ok, later_ok,
                    block_send, block_recv, data_send, data_recv, leaf_send, leaf_recv):
    f, d = lax.axis_index('feat'), lax.axis_index('data')
    x, core = d // 2, d % 2
    chief, other = 2 * x + 1, 2 * x + 1 - core
    near = x + 1 - 2 * (x % 2)
    lines = [near, (x + 2) % SIDE, SIDE - 1 - x]
    data_peers = [other] + [2 * line + c for c in (1, 0) for line in lines]
    rank = sum(jnp.where(f == peer, FEAT_RANK[peer], 0) for peer in range(NF))
    is_chief = core == 1

    own = pltpu.make_async_copy(bin_hbm, values.at[1, f], block_recv.at[1])
    local = [
        pltpu.make_async_copy(bin_hbm, own_bins, local_sem.at[0]),
        pltpu.make_async_copy(grad_hbm, own_grad, local_sem.at[1]),
        pltpu.make_async_copy(hess_hbm, own_hess, local_sem.at[2]),
        pltpu.make_async_copy(feat_hbm, feat_in, local_sem.at[3]),
        pltpu.make_async_copy(thr_hbm, thr_in, local_sem.at[4]),
        pltpu.make_async_copy(reg_hbm, reg_in, local_sem.at[5]),
    ]
    barrier = pltpu.get_barrier_semaphore()

    def signal(semaphore, **device):
        pl.semaphore_signal(semaphore, inc=1, device_id=device, device_id_type=MESH)

    def send_block(peer, group):
        pltpu.make_async_remote_copy(
            src_ref=bin_hbm, dst_ref=values.at[group, f], send_sem=block_send, recv_sem=block_recv.at[group],
            device_id={'feat': peer, 'data': chief}, device_id_type=MESH).start()

    @pl.when(is_chief)
    def _():
        for peer in reversed(FEAT_ORDER):
            pl.when(FEAT_RANK[peer] > rank)(lambda: signal(barrier, feat=peer))
        signal(barrier, data=other)
        own.start()

    @pl.when(jnp.logical_not(is_chief))
    def _():
        signal(barrier, data=other)

        @pl.when(d == HUB)
        def _():
            for peer in range(2, ND, 2):
                signal(barrier, data=peer)
    for copy in local:
        copy.start()

    @pl.when(is_chief)
    def _():
        pl.semaphore_wait(barrier, rank + 1)
        signal(earlier_ok, data=other)
        for peer in SEND_ORDER:
            pl.when(FEAT_RANK[peer] < rank)(lambda: send_block(peer, 1))
        own_group = sum(jnp.where(rank >= first, 1, 0) for first, _ in RANK_GROUPS) - 1
        for peer in FEAT_ORDER:
            pl.when(FEAT_RANK[peer] < rank)(lambda: signal(ready.at[own_group], feat=peer))

    @pl.when(jnp.logical_not(is_chief))
    def _():
        pl.semaphore_wait(barrier, jnp.where(d == HUB, 1, 2))
        pl.when(d != HUB)(lambda: signal(gathered, data=HUB))
        pl.semaphore_wait(earlier_ok, 1)
        for peer in SEND_ORDER:
            pl.when(FEAT_RANK[peer] <= rank)(lambda: send_block(peer, 0))

    for copy in local:
        copy.wait()
    for peer in range(ND):
        parcels[peer, 0] = own_bins[peer:peer + 1, :].astype(jnp.float32)
        parcels[peer, 1] = own_grad[...]
        parcels[peer, 2] = own_hess[...]
    rows[d] = parcels[d]

    @pl.when(d == HUB)
    def _():
        pl.semaphore_wait(gathered, SIDE - 1)
        for peer in data_peers:
            signal(everyone, data=peer)

    @pl.when(d != HUB)
    def _():
        pl.semaphore_wait(everyone, 1)
    for peer in data_peers:
        pltpu.make_async_remote_copy(
            src_ref=parcels.at[peer], dst_ref=rows.at[d], send_sem=data_send, recv_sem=data_recv,
            device_id={'data': peer}, device_id_type=MESH).start()

    for group, (first, last) in enumerate(RANK_GROUPS):
        count = last - jnp.maximum(rank, first - 1)

        @pl.when(is_chief & (count > 0))
        def _():
            pl.semaphore_wait(ready.at[group], count)
            signal(later_ok, data=other)
            for peer in FEAT_ORDER[first:last + 1]:
                pl.when(FEAT_RANK[peer] > rank)(lambda: send_block(peer, 1))

        @pl.when(jnp.logical_not(is_chief) & (count > 0))
        def _():
            pl.semaphore_wait(later_ok, 1)
            for peer in FEAT_ORDER[first:last + 1]:
                pl.when(FEAT_RANK[peer] > rank)(lambda: send_block(peer, 0))

    reg_row[...] = jnp.broadcast_to(reg_in[0], (1, 128))
    zero = jnp.float32(0)
    sources = [chief, chief - 1] + data_peers[1:]

    @pl.when(is_chief)
    def _():
        feat_tbl[...] = jnp.zeros_like(feat_tbl)
        thr_tbl[...] = jnp.zeros_like(thr_tbl)
        feat_tbl[0:7, 0:64] = feat_in[...]
        thr_tbl[0:7, 0:64] = thr_in[...]
        select, threshold = node_tables(feat_tbl[...], thr_tbl[...])
        for group in (1, 0):
            block = values.at[group]
            pltpu.make_async_copy(block, block, block_recv.at[group]).wait()
            s = chief - 1 + group
            table = values[group].reshape(NF * 8, CHUNK).astype(jnp.float32).astype(jnp.bfloat16)
            leaves[s] = route(table, select, threshold)
            for peer in DATA_ORDER:
                @pl.when(peer != d)
                def _():
                    pltpu.make_async_remote_copy(
                        src_ref=leaves.at[s], dst_ref=leaves.at[s], send_sem=leaf_send, recv_sem=leaf_recv.at[s],
                        device_id={'data': peer}, device_id_type=MESH).start()

    arrived = rows.at[pl.ds(0, ND - 1)]
    pltpu.make_async_copy(arrived, arrived, data_recv).wait()
    columns[...] = jnp.concatenate([rows[s, 0] for s in sources], axis=0).T

    def build(k):
        below[k] = jnp.where(columns[:, k:k + 1] <= iota((CHUNK, NBINS), 1).astype(jnp.float32), jnp.float32(1), zero).astype(jnp.bfloat16)

    totals = [None, None]
    for k, s in enumerate(sources):
        for later in BUILD.get(k, ()):
            build(later)
        arrival = pltpu.make_async_copy(leaves.at[s], leaves.at[s], leaf_recv.at[s])
        if k < 2:
            pl.when(jnp.logical_not(is_chief))(arrival.wait)
        else:
            arrival.wait()
        member = leaves[s] == iota((LEAVES, CHUNK), 0)
        mark = jnp.where(member, jnp.float32(1), zero).astype(jnp.bfloat16)
        for part in range(2):
            value = rows[s, 1 + part]
            inside = jnp.where(member, value, zero)
            leaf_sums[s, part] = inside[:, :128] + inside[:, 128:256] + (inside[:, 256:384] + inside[:, 384:])
            product = jnp.dot(jnp.concatenate([mark * piece for piece in split3(value)], axis=0), below[k], preferred_element_type=jnp.float32)
            product = product[:LEAVES] + product[LEAVES:2 * LEAVES] + product[2 * LEAVES:]
            totals[part] = product if k == 0 else totals[part] + product
    leaf_total = []
    for part in range(2):
        whole = leaf_sums[0, part]
        for s in range(1, ND):
            whole = whole + leaf_sums[s, part]
        leaf_total.append(jnp.sum(whole.T, axis=0, keepdims=True))
    leaf_row[...] = -leaf_total[0] / (leaf_total[1] + reg_row[...])
    for part in range(2):
        for half in range(2):
            sums[part, half] = totals[part][:, 128 * half:128 * (half + 1)]

    @pl.when(is_chief)
    def _():
        sent = values.at[0, pl.ds(0, NF - 1)]
        pltpu.make_async_copy(sent, sent, block_send).wait()
        told = leaves.at[pl.ds(0, ND - 1)]
        pltpu.make_async_copy(told, told, leaf_send).wait()
        pltpu.make_async_copy(told, told, leaf_send).wait()

    @pl.when(jnp.logical_not(is_chief))
    def _():
        sent = values.at[0]
        pltpu.make_async_copy(sent, sent, block_send).wait()
    pltpu.make_async_copy(arrived, arrived, data_send).wait()


def gain_kernel(reg_row, sums, leaf_row, gain_hbm, leaf_hbm, heap, gains, out_sem):
    reg = reg_row[...]

    def score(g, h):
        return g * g / (h + reg)

    def fill(source, first, start, count):
        for r in range(start, start + count, 8):
            n = min(8, start + count - r)
            rows = pl.ds(r - first, n)
            all_g = source[0, 1, rows, 127:128]
            all_h = source[1, 1, rows, 127:128]
            whole = score(all_g, all_h)
            for half in range(2):
                left_g, left_h = source[0, half, rows, :], source[1, half, rows, :]
                gain = 0.5 * (score(left_g, left_h) + score(all_g - left_g, all_h - left_h) - whole)
                wide = 128 - half
                gains[pl.ds(r, n), 0, pl.ds(128 * half, wide)] = gain[:, :wide]
        pltpu.make_async_copy(gains.at[pl.ds(start, count)], gain_hbm.at[pl.ds(start, count)], out_sem.at[0]).start()

    leaf_copy = pltpu.make_async_copy(leaf_row, leaf_hbm, out_sem.at[1])
    leaf_copy.start()
    for level in range(6, -1, -1):
        n = 2 ** level
        source, base = (sums, 0) if level == 6 else (heap, 2 * n)
        for part in range(2):
            for half in range(2):
                heap[part, half, n:2 * n, :] = (source[part, half, pl.ds(base, n, stride=2), :]
                                                + source[part, half, pl.ds(base + 1, n, stride=2), :])
    fill(heap, -1, 0, 127)
    fill(sums, 127, 127, 64)
    fill(sums, 127, 191, 64)
    leaf_copy.wait()
    pltpu.make_async_copy(gains, gain_hbm, out_sem.at[0]).wait()


def solution(mesh):
    def per_device(binned, gradient, hessian, split_feat, split_thr, reg_lambda):
        hbm = pl.BlockSpec(memory_space=pltpu.HBM)
        vmem = pl.BlockSpec(memory_space=pltpu.VMEM)
        dma, regular = pltpu.SemaphoreType.DMA, pltpu.SemaphoreType.REGULAR
        inputs = [binned.T, gradient.reshape(1, CHUNK), hessian.reshape(1, CHUNK), split_feat, split_thr]
        sums, leaf_row, reg_row = pl.pallas_call(
            exchange_kernel,
            out_shape=[
                jax.ShapeDtypeStruct((2, 2, LEAVES, 128), jnp.float32),
                jax.ShapeDtypeStruct((1, LEAVES), jnp.float32),
                jax.ShapeDtypeStruct((1, 128), jnp.float32),
            ],
            in_specs=[hbm] * 5 + [pl.BlockSpec(memory_space=pl.ANY)],
            out_specs=[vmem] * 3,
            scratch_shapes=[
                pltpu.VMEM((ND, 2, LEAVES, 128), jnp.float32),
                pltpu.VMEM((2, NF, 8, CHUNK), jnp.int32),
                pltpu.VMEM((ND, 3, 1, CHUNK), jnp.float32),
                pltpu.VMEM((ND, 3, 1, CHUNK), jnp.float32),
                pltpu.VMEM((CHUNK, ND), jnp.float32),
                pltpu.VMEM((ND, 1, CHUNK), jnp.int32),
                pltpu.VMEM((ND, CHUNK, NBINS), jnp.bfloat16),
                pltpu.VMEM((8, CHUNK), jnp.int32),
                pltpu.VMEM((1, CHUNK), jnp.float32),
                pltpu.VMEM((1, CHUNK), jnp.float32),
                pltpu.SMEM((1,), jnp.float32),
                pltpu.VMEM((7, 64), jnp.int32),
                pltpu.VMEM((7, 64), jnp.int32),
                pltpu.VMEM((8, 128), jnp.int32),
                pltpu.VMEM((8, 128), jnp.int32),
                dma((6,)), regular((len(RANK_GROUPS),)), regular, regular, regular, regular,
                dma, dma((2,)), dma, dma, dma, dma((ND,)),
            ],
            compiler_params=pltpu.CompilerParams(collective_id=0, has_side_effects=True, vmem_limit_bytes=24 * 2 ** 20),
            name='exchange',
        )(*[pltpu.with_memory_space_constraint(a, pltpu.HBM) for a in inputs], reg_lambda)
        gain, leaf_value = pl.pallas_call(
            gain_kernel,
            out_shape=[
                jax.ShapeDtypeStruct((255, 1, 255), jnp.float32),
                jax.ShapeDtypeStruct((1, LEAVES), jnp.float32),
            ],
            in_specs=[vmem] * 3,
            out_specs=[hbm] * 2,
            scratch_shapes=[
                pltpu.VMEM((2, 2, LEAVES, 128), jnp.float32),
                pltpu.VMEM((255, 1, 255), jnp.float32),
                dma((2,)),
            ],
            compiler_params=pltpu.CompilerParams(vmem_limit_bytes=24 * 2 ** 20),
            name='gains',
        )(reg_row, sums, leaf_row)
        return gain, leaf_value.reshape(LEAVES)

    row_spec = P(('tree', 'data'))
    return jax.shard_map(
        per_device,
        mesh=mesh,
        in_specs=(P(('tree', 'data'), 'feat'), row_spec, row_spec, P('tree', None), P('tree', None), P(None)),
        out_specs=(P('tree', ('feat', 'data'), None), P('tree')),
        check_vma=False,
    )
```

```python
import jax
import jax.numpy as jnp
from jax import lax
from jax.experimental import pallas as pl
from jax.experimental.pallas import tpu as pltpu
from jax.sharding import PartitionSpec as P

NBINS = 256
SIDE = 4
NF = SIDE * SIDE
ND = 8
CHUNK = 512
LEAVES = 128
HUB = 0
FEAT_ORDER = (0, 1, 2, 4, 3, 8, 9, 7, 5, 12, 6, 10, 11, 14, 13, 15)
FEAT_RANK = [FEAT_ORDER.index(f) for f in range(NF)]
BUILD = {0: (0,), 1: (1,), 2: (2, 3), 3: (4, 5, 6, 7)}
SEND_ORDER = (0, 8, 15, 3, 2, 13, 4, 1, 5, 14, 7, 9, 11, 6, 12, 10)
RANK_GROUPS = ((0, 7), (8, 15))
DATA_ORDER = (1, 0, 3, 2, 5, 4, 7, 6)
MESH = pl.DeviceIdType.MESH


def split3(value):
    largest = float(jnp.finfo(jnp.bfloat16).max)
    first = jnp.clip(value, -largest, largest).astype(jnp.bfloat16)
    rest = value - first.astype(jnp.float32)
    second = rest.astype(jnp.bfloat16)
    third = (rest - second.astype(jnp.float32)).astype(jnp.bfloat16)
    return first, second, third


def iota(shape, dim):
    return lax.broadcasted_iota(jnp.int32, shape, dim)


def contract_lanes(left, right):
    return lax.dot_general(left, right, (((1,), (1,)), ((), ())), preferred_element_type=jnp.float32)


def node_tables(feat_tbl, thr_tbl):
    lane = iota((8, 128), 1)
    feat_row = jnp.zeros((1, 128), jnp.int32)
    thr_row = jnp.zeros((1, 128), jnp.int32)
    for level in range(7):
        here = (lane >= 2 ** level) & (lane < 2 ** (level + 1))
        feat_row = feat_row + jnp.where(here, pltpu.roll(feat_tbl, 2 ** level, 1), 0)[level:level + 1]
        thr_row = thr_row + jnp.where(here, pltpu.roll(thr_tbl, 2 ** level, 1), 0)[level:level + 1]
    one, zero = jnp.float32(1), jnp.float32(0)
    by_feat = jnp.where(feat_row == iota((128, 128), 0), one, zero).astype(jnp.bfloat16)
    by_thr = jnp.broadcast_to(thr_row.astype(jnp.float32), (128, 128)).astype(jnp.bfloat16)
    position = iota((128, 128), 0)
    reverse = jnp.zeros((128, 128), jnp.int32)
    for bit in range(7):
        reverse = reverse | (((position >> bit) & 1) << (6 - bit))
    heap = jnp.zeros((128, 128), jnp.int32)
    for level in range(7):
        heap = jnp.where(position >= 2 ** level, 2 ** level + (reverse >> (7 - level)), heap)
    order = jnp.where(heap == iota((128, 128), 1), one, zero).astype(jnp.bfloat16)
    return contract_lanes(order, by_feat).astype(jnp.bfloat16), contract_lanes(order, by_thr)


def route(values, select, threshold):
    picked = jnp.dot(select, values, preferred_element_type=jnp.float32)
    limit = jnp.concatenate([threshold] * (values.shape[1] // 128), axis=1)
    right = picked > limit
    leaf = jnp.where(right[64:128], 1, 0)
    for level in range(5, -1, -1):
        n = 2 ** level
        leaf = jnp.where(right[n:2 * n], leaf[n:] + 2 ** (6 - level), leaf[:n])
    return leaf


def exchange_kernel(*refs):
    dma, regular = pltpu.SemaphoreType.DMA, pltpu.SemaphoreType.REGULAR
    pl.run_scoped(
        lambda *own: exchange(*refs, *own),
        regular((len(RANK_GROUPS),)), regular, regular, regular, regular,
        dma((2,)), dma, dma((ND,)), dma((6,)), dma, dma, dma)


def exchange(bin_hbm, grad_hbm, hess_hbm, feat_hbm, thr_hbm, reg_hbm, sums, leaf_row, reg_row,
                    leaf_sums, values, parcels, rows, columns, leaves, below, own_bins, own_grad, own_hess, reg_in, feat_in, thr_in, feat_tbl, thr_tbl,
                    ready, gathered, everyone, earlier_ok, later_ok, block_recv, data_recv, leaf_recv,
                    local_sem, block_send, data_send, leaf_send):
    f, d = lax.axis_index('feat'), lax.axis_index('data')
    x, core = d // 2, d % 2
    chief, other = 2 * x + 1, 2 * x + 1 - core
    near = x + 1 - 2 * (x % 2)
    lines = [near, (x + 2) % SIDE, SIDE - 1 - x]
    data_peers = [other] + [2 * line + c for c in (1, 0) for line in lines]
    rank = sum(jnp.where(f == peer, FEAT_RANK[peer], 0) for peer in range(NF))
    is_chief = core == 1

    own = pltpu.make_async_copy(bin_hbm, values.at[1, f], block_recv.at[1])
    local = [
        pltpu.make_async_copy(bin_hbm, own_bins, local_sem.at[0]),
        pltpu.make_async_copy(grad_hbm, own_grad, local_sem.at[1]),
        pltpu.make_async_copy(hess_hbm, own_hess, local_sem.at[2]),
        pltpu.make_async_copy(feat_hbm, feat_in, local_sem.at[3]),
        pltpu.make_async_copy(thr_hbm, thr_in, local_sem.at[4]),
        pltpu.make_async_copy(reg_hbm, reg_in, local_sem.at[5]),
    ]
    barrier = pltpu.get_barrier_semaphore()

    def signal(semaphore, **device):
        pl.semaphore_signal(semaphore, inc=1, device_id=device, device_id_type=MESH)

    def send_block(peer, group):
        pltpu.make_async_remote_copy(
            src_ref=bin_hbm, dst_ref=values.at[group, f], send_sem=block_send, recv_sem=block_recv.at[group],
            device_id={'feat': peer, 'data': chief}, device_id_type=MESH).start()

    @pl.when(is_chief)
    def _():
        for peer in reversed(FEAT_ORDER):
            pl.when(FEAT_RANK[peer] > rank)(lambda: signal(barrier, feat=peer))
        signal(barrier, data=other)
        own.start()

    @pl.when(jnp.logical_not(is_chief))
    def _():
        signal(barrier, data=other)

        @pl.when(d == HUB)
        def _():
            for peer in range(2, ND, 2):
                signal(barrier, data=peer)
    for copy in local:
        copy.start()

    @pl.when(is_chief)
    def _():
        pl.semaphore_wait(barrier, rank + 1)
        signal(earlier_ok, data=other)
        for peer in SEND_ORDER:
            pl.when(FEAT_RANK[peer] < rank)(lambda: send_block(peer, 1))
        own_group = sum(jnp.where(rank >= first, 1, 0) for first, _ in RANK_GROUPS) - 1
        for peer in FEAT_ORDER:
            pl.when(FEAT_RANK[peer] < rank)(lambda: signal(ready.at[own_group], feat=peer))

    @pl.when(jnp.logical_not(is_chief))
    def _():
        pl.semaphore_wait(barrier, jnp.where(d == HUB, 1, 2))
        pl.when(d != HUB)(lambda: signal(gathered, data=HUB))
        pl.semaphore_wait(earlier_ok, 1)
        for peer in SEND_ORDER:
            pl.when(FEAT_RANK[peer] <= rank)(lambda: send_block(peer, 0))

    for copy in local:
        copy.wait()
    for peer in range(ND):
        parcels[peer, 0] = own_bins[peer:peer + 1, :].astype(jnp.float32)
        parcels[peer, 1] = own_grad[...]
        parcels[peer, 2] = own_hess[...]
    rows[d] = parcels[d]

    @pl.when(d == HUB)
    def _():
        pl.semaphore_wait(gathered, SIDE - 1)
        for peer in data_peers:
            signal(everyone, data=peer)

    @pl.when(d != HUB)
    def _():
        pl.semaphore_wait(everyone, 1)
    for peer in data_peers:
        pltpu.make_async_remote_copy(
            src_ref=parcels.at[peer], dst_ref=rows.at[d], send_sem=data_send, recv_sem=data_recv,
            device_id={'data': peer}, device_id_type=MESH).start()

    for group, (first, last) in enumerate(RANK_GROUPS):
        count = last - jnp.maximum(rank, first - 1)

        @pl.when(is_chief & (count > 0))
        def _():
            pl.semaphore_wait(ready.at[group], count)
            signal(later_ok, data=other)
            for peer in FEAT_ORDER[first:last + 1]:
                pl.when(FEAT_RANK[peer] > rank)(lambda: send_block(peer, 1))

        @pl.when(jnp.logical_not(is_chief) & (count > 0))
        def _():
            pl.semaphore_wait(later_ok, 1)
            for peer in FEAT_ORDER[first:last + 1]:
                pl.when(FEAT_RANK[peer] > rank)(lambda: send_block(peer, 0))

    reg_row[...] = jnp.broadcast_to(reg_in[0], (1, 128))
    zero = jnp.float32(0)
    sources = [chief, chief - 1] + data_peers[1:]

    @pl.when(is_chief)
    def _():
        feat_tbl[...] = jnp.zeros_like(feat_tbl)
        thr_tbl[...] = jnp.zeros_like(thr_tbl)
        feat_tbl[0:7, 0:64] = feat_in[...]
        thr_tbl[0:7, 0:64] = thr_in[...]
        select, threshold = node_tables(feat_tbl[...], thr_tbl[...])
        for group in (1, 0):
            block = values.at[group]
            pltpu.make_async_copy(block, block, block_recv.at[group]).wait()
            s = chief - 1 + group
            table = values[group].reshape(NF * 8, CHUNK).astype(jnp.float32).astype(jnp.bfloat16)
            leaves[s] = route(table, select, threshold)
            for peer in DATA_ORDER:
                @pl.when(peer != d)
                def _():
                    pltpu.make_async_remote_copy(
                        src_ref=leaves.at[s], dst_ref=leaves.at[s], send_sem=leaf_send, recv_sem=leaf_recv.at[s],
                        device_id={'data': peer}, device_id_type=MESH).start()

    arrived = rows.at[pl.ds(0, ND - 1)]
    pltpu.make_async_copy(arrived, arrived, data_recv).wait()
    columns[...] = jnp.concatenate([rows[s, 0] for s in sources], axis=0).T

    def build(k):
        below[k] = jnp.where(columns[:, k:k + 1] <= iota((CHUNK, NBINS), 1).astype(jnp.float32), jnp.float32(1), zero).astype(jnp.bfloat16)

    totals = [None, None]
    for k, s in enumerate(sources):
        for later in BUILD.get(k, ()):
            build(later)
        arrival = pltpu.make_async_copy(leaves.at[s], leaves.at[s], leaf_recv.at[s])
        if k < 2:
            pl.when(jnp.logical_not(is_chief))(arrival.wait)
        else:
            arrival.wait()
        member = leaves[s] == iota((LEAVES, CHUNK), 0)
        mark = jnp.where(member, jnp.float32(1), zero).astype(jnp.bfloat16)
        for part in range(2):
            value = rows[s, 1 + part]
            inside = jnp.where(member, value, zero)
            leaf_sums[s, part] = inside[:, :128] + inside[:, 128:256] + (inside[:, 256:384] + inside[:, 384:])
            product = jnp.dot(jnp.concatenate([mark * piece for piece in split3(value)], axis=0), below[k], preferred_element_type=jnp.float32)
            product = product[:LEAVES] + product[LEAVES:2 * LEAVES] + product[2 * LEAVES:]
            totals[part] = product if k == 0 else totals[part] + product
    leaf_total = []
    for part in range(2):
        whole = leaf_sums[0, part]
        for s in range(1, ND):
            whole = whole + leaf_sums[s, part]
        leaf_total.append(jnp.sum(whole.T, axis=0, keepdims=True))
    leaf_row[...] = -leaf_total[0] / (leaf_total[1] + reg_row[...])
    for part in range(2):
        for half in range(2):
            sums[part, half] = totals[part][:, 128 * half:128 * (half + 1)]

    @pl.when(is_chief)
    def _():
        sent = values.at[0, pl.ds(0, NF - 1)]
        pltpu.make_async_copy(sent, sent, block_send).wait()
        told = leaves.at[pl.ds(0, ND - 1)]
        pltpu.make_async_copy(told, told, leaf_send).wait()
        pltpu.make_async_copy(told, told, leaf_send).wait()

    @pl.when(jnp.logical_not(is_chief))
    def _():
        sent = values.at[0]
        pltpu.make_async_copy(sent, sent, block_send).wait()
    pltpu.make_async_copy(arrived, arrived, data_send).wait()


def gain_kernel(*refs):
    pl.run_scoped(lambda out_sem: fill_gains(*refs, out_sem), pltpu.SemaphoreType.DMA((2,)))


def fill_gains(reg_row, sums, leaf_row, gain_hbm, leaf_hbm, heap, gains, out_sem):
    reg = reg_row[...]

    def score(g, h):
        return g * g / (h + reg)

    def fill(source, first, start, count):
        for r in range(start, start + count, 8):
            n = min(8, start + count - r)
            rows = pl.ds(r - first, n)
            all_g = source[0, 1, rows, 127:128]
            all_h = source[1, 1, rows, 127:128]
            whole = score(all_g, all_h)
            for half in range(2):
                left_g, left_h = source[0, half, rows, :], source[1, half, rows, :]
                gain = 0.5 * (score(left_g, left_h) + score(all_g - left_g, all_h - left_h) - whole)
                wide = 128 - half
                gains[pl.ds(r, n), 0, pl.ds(128 * half, wide)] = gain[:, :wide]
        pltpu.make_async_copy(gains.at[pl.ds(start, count)], gain_hbm.at[pl.ds(start, count)], out_sem.at[0]).start()

    leaf_copy = pltpu.make_async_copy(leaf_row, leaf_hbm, out_sem.at[1])
    leaf_copy.start()
    for level in range(6, -1, -1):
        n = 2 ** level
        source, base = (sums, 0) if level == 6 else (heap, 2 * n)
        for part in range(2):
            for half in range(2):
                heap[part, half, n:2 * n, :] = (source[part, half, pl.ds(base, n, stride=2), :]
                                                + source[part, half, pl.ds(base + 1, n, stride=2), :])
    fill(heap, -1, 0, 127)
    fill(sums, 127, 127, 64)
    fill(sums, 127, 191, 64)
    leaf_copy.wait()
    pltpu.make_async_copy(gains, gain_hbm, out_sem.at[0]).wait()


def solution(mesh):
    def per_device(binned, gradient, hessian, split_feat, split_thr, reg_lambda):
        hbm = pl.BlockSpec(memory_space=pltpu.HBM)
        vmem = pl.BlockSpec(memory_space=pltpu.VMEM)
        inputs = [binned.T, gradient.reshape(1, CHUNK), hessian.reshape(1, CHUNK), split_feat, split_thr]
        sums, leaf_row, reg_row = pl.pallas_call(
            exchange_kernel,
            out_shape=[
                jax.ShapeDtypeStruct((2, 2, LEAVES, 128), jnp.float32),
                jax.ShapeDtypeStruct((1, LEAVES), jnp.float32),
                jax.ShapeDtypeStruct((1, 128), jnp.float32),
            ],
            in_specs=[hbm] * 5 + [pl.BlockSpec(memory_space=pl.ANY)],
            out_specs=[vmem] * 3,
            scratch_shapes=[
                pltpu.VMEM((ND, 2, LEAVES, 128), jnp.float32),
                pltpu.VMEM((2, NF, 8, CHUNK), jnp.int32),
                pltpu.VMEM((ND, 3, 1, CHUNK), jnp.float32),
                pltpu.VMEM((ND, 3, 1, CHUNK), jnp.float32),
                pltpu.VMEM((CHUNK, ND), jnp.float32),
                pltpu.VMEM((ND, 1, CHUNK), jnp.int32),
                pltpu.VMEM((ND, CHUNK, NBINS), jnp.bfloat16),
                pltpu.VMEM((8, CHUNK), jnp.int32),
                pltpu.VMEM((1, CHUNK), jnp.float32),
                pltpu.VMEM((1, CHUNK), jnp.float32),
                pltpu.SMEM((1,), jnp.float32),
                pltpu.VMEM((7, 64), jnp.int32),
                pltpu.VMEM((7, 64), jnp.int32),
                pltpu.VMEM((8, 128), jnp.int32),
                pltpu.VMEM((8, 128), jnp.int32),
            ],
            compiler_params=pltpu.CompilerParams(collective_id=0, has_side_effects=True, vmem_limit_bytes=24 * 2 ** 20),
            name='exchange',
        )(*[pltpu.with_memory_space_constraint(a, pltpu.HBM) for a in inputs], reg_lambda)
        gain, leaf_value = pl.pallas_call(
            gain_kernel,
            out_shape=[
                jax.ShapeDtypeStruct((255, 1, 255), jnp.float32),
                jax.ShapeDtypeStruct((1, LEAVES), jnp.float32),
            ],
            in_specs=[vmem] * 3,
            out_specs=[hbm] * 2,
            scratch_shapes=[
                pltpu.VMEM((2, 2, LEAVES, 128), jnp.float32),
                pltpu.VMEM((255, 1, 255), jnp.float32),
            ],
            compiler_params=pltpu.CompilerParams(vmem_limit_bytes=24 * 2 ** 20),
            name='gains',
        )(reg_row, sums, leaf_row)
        return gain, leaf_value.reshape(LEAVES)

    row_spec = P(('tree', 'data'))
    return jax.shard_map(
        per_device,
        mesh=mesh,
        in_specs=(P(('tree', 'data'), 'feat'), row_spec, row_spec, P('tree', None), P('tree', None), P(None)),
        out_specs=(P('tree', ('feat', 'data'), None), P('tree')),
        check_vma=False,
    )
```

```python
import jax
import jax.numpy as jnp
from jax import lax
from jax.experimental import pallas as pl
from jax.experimental.pallas import tpu as pltpu
from jax.sharding import PartitionSpec as P

NBINS = 256
SIDE = 4
NF = SIDE * SIDE
ND = 8
CHUNK = 512
LEAVES = 128
HUB = 0
FEAT_ORDER = (0, 1, 2, 4, 3, 8, 9, 7, 5, 12, 6, 10, 11, 14, 13, 15)
FEAT_RANK = [FEAT_ORDER.index(f) for f in range(NF)]
BUILD = {0: (0,), 1: (1,), 2: (2, 3), 3: (4, 5, 6, 7)}
SEND_ORDER = (0, 8, 15, 3, 2, 13, 4, 1, 5, 14, 7, 9, 11, 6, 12, 10)
RANK_GROUPS = ((0, 7), (8, 15))
DATA_ORDER = (1, 0, 3, 2, 5, 4, 7, 6)
MESH = pl.DeviceIdType.MESH


def split3(value):
    largest = float(jnp.finfo(jnp.bfloat16).max)
    first = jnp.clip(value, -largest, largest).astype(jnp.bfloat16)
    rest = value - first.astype(jnp.float32)
    second = rest.astype(jnp.bfloat16)
    third = (rest - second.astype(jnp.float32)).astype(jnp.bfloat16)
    return first, second, third


def iota(shape, dim):
    return lax.broadcasted_iota(jnp.int32, shape, dim)


def contract_lanes(left, right):
    return lax.dot_general(left, right, (((1,), (1,)), ((), ())), preferred_element_type=jnp.float32)


def node_tables(feat_tbl, thr_tbl):
    lane = iota((8, 128), 1)
    feat_row = jnp.zeros((1, 128), jnp.int32)
    thr_row = jnp.zeros((1, 128), jnp.int32)
    for level in range(7):
        here = (lane >= 2 ** level) & (lane < 2 ** (level + 1))
        feat_row = feat_row + jnp.where(here, pltpu.roll(feat_tbl, 2 ** level, 1), 0)[level:level + 1]
        thr_row = thr_row + jnp.where(here, pltpu.roll(thr_tbl, 2 ** level, 1), 0)[level:level + 1]
    one, zero = jnp.float32(1), jnp.float32(0)
    by_feat = jnp.where(feat_row == iota((128, 128), 0), one, zero).astype(jnp.bfloat16)
    by_thr = jnp.broadcast_to(thr_row.astype(jnp.float32), (128, 128)).astype(jnp.bfloat16)
    position = iota((128, 128), 0)
    reverse = jnp.zeros((128, 128), jnp.int32)
    for bit in range(7):
        reverse = reverse | (((position >> bit) & 1) << (6 - bit))
    heap = jnp.zeros((128, 128), jnp.int32)
    for level in range(7):
        heap = jnp.where(position >= 2 ** level, 2 ** level + (reverse >> (7 - level)), heap)
    order = jnp.where(heap == iota((128, 128), 1), one, zero).astype(jnp.bfloat16)
    return contract_lanes(order, by_feat).astype(jnp.bfloat16), contract_lanes(order, by_thr)


def route(values, select, threshold):
    picked = jnp.dot(select, values, preferred_element_type=jnp.float32)
    limit = jnp.concatenate([threshold] * (values.shape[1] // 128), axis=1)
    right = picked > limit
    leaf = jnp.where(right[64:128], 1, 0)
    for level in range(5, -1, -1):
        n = 2 ** level
        leaf = jnp.where(right[n:2 * n], leaf[n:] + 2 ** (6 - level), leaf[:n])
    return leaf


def exchange_kernel(*refs):
    dma, regular = pltpu.SemaphoreType.DMA, pltpu.SemaphoreType.REGULAR
    pl.run_scoped(
        lambda *own: exchange(*refs, *own),
        regular((len(RANK_GROUPS),)), regular, regular, regular, regular,
        dma((2,)), dma, dma((ND,)), dma((6,)), dma, dma, dma)


def exchange(bin_hbm, grad_hbm, hess_hbm, feat_hbm, thr_hbm, reg_hbm, sums, leaf_row, reg_row,
                    leaf_sums, values, parcels, rows, columns, leaves, below, own_bins, own_grad, own_hess, reg_in, feat_in, thr_in, feat_tbl, thr_tbl,
                    ready, gathered, everyone, earlier_ok, later_ok, block_recv, data_recv, leaf_recv,
                    local_sem, block_send, data_send, leaf_send):
    f, d = lax.axis_index('feat'), lax.axis_index('data')
    x, core = d // 2, d % 2
    chief, other = 2 * x + 1, 2 * x + 1 - core
    near = x + 1 - 2 * (x % 2)
    lines = [near, (x + 2) % SIDE, SIDE - 1 - x]
    data_peers = [other] + [2 * line + c for c in (1, 0) for line in lines]
    rank = sum(jnp.where(f == peer, FEAT_RANK[peer], 0) for peer in range(NF))
    is_chief = core == 1

    own = pltpu.make_async_copy(bin_hbm, values.at[1, f], block_recv.at[1])
    local = [
        pltpu.make_async_copy(bin_hbm, own_bins, local_sem.at[0]),
        pltpu.make_async_copy(grad_hbm, own_grad, local_sem.at[1]),
        pltpu.make_async_copy(hess_hbm, own_hess, local_sem.at[2]),
        pltpu.make_async_copy(feat_hbm, feat_in, local_sem.at[3]),
        pltpu.make_async_copy(thr_hbm, thr_in, local_sem.at[4]),
        pltpu.make_async_copy(reg_hbm, reg_in, local_sem.at[5]),
    ]
    barrier = pltpu.get_barrier_semaphore()

    def signal(semaphore, **device):
        pl.semaphore_signal(semaphore, inc=1, device_id=device, device_id_type=MESH)

    def send_block(peer, group):
        pltpu.make_async_remote_copy(
            src_ref=bin_hbm, dst_ref=values.at[group, f], send_sem=block_send, recv_sem=block_recv.at[group],
            device_id={'feat': peer, 'data': chief}, device_id_type=MESH).start()

    @pl.when(is_chief)
    def _():
        for peer in reversed(FEAT_ORDER):
            pl.when(FEAT_RANK[peer] > rank)(lambda: signal(barrier, feat=peer))
        signal(barrier, data=other)
        own.start()

    @pl.when(jnp.logical_not(is_chief))
    def _():
        signal(barrier, data=other)

        @pl.when(d == HUB)
        def _():
            for peer in range(2, ND, 2):
                signal(barrier, data=peer)
    for copy in local:
        copy.start()

    @pl.when(is_chief)
    def _():
        pl.semaphore_wait(barrier, rank + 1)
        signal(earlier_ok, data=other)
        for peer in SEND_ORDER:
            pl.when(FEAT_RANK[peer] < rank)(lambda: send_block(peer, 1))
        own_group = sum(jnp.where(rank >= first, 1, 0) for first, _ in RANK_GROUPS) - 1
        for peer in FEAT_ORDER:
            pl.when(FEAT_RANK[peer] < rank)(lambda: signal(ready.at[own_group], feat=peer))

    @pl.when(jnp.logical_not(is_chief))
    def _():
        pl.semaphore_wait(barrier, jnp.where(d == HUB, 1, 2))
        pl.when(d != HUB)(lambda: signal(gathered, data=HUB))
        pl.semaphore_wait(earlier_ok, 1)
        for peer in SEND_ORDER:
            pl.when(FEAT_RANK[peer] <= rank)(lambda: send_block(peer, 0))

    for copy in local:
        copy.wait()
    for peer in range(ND):
        parcels[peer, 0] = own_bins[peer:peer + 1, :].astype(jnp.float32)
        parcels[peer, 1] = own_grad[...]
        parcels[peer, 2] = own_hess[...]
    rows[d] = parcels[d]

    @pl.when(d == HUB)
    def _():
        pl.semaphore_wait(gathered, SIDE - 1)
        for peer in data_peers:
            signal(everyone, data=peer)

    @pl.when(d != HUB)
    def _():
        pl.semaphore_wait(everyone, 1)
    for peer in data_peers:
        pltpu.make_async_remote_copy(
            src_ref=parcels.at[peer], dst_ref=rows.at[d], send_sem=data_send, recv_sem=data_recv,
            device_id={'data': peer}, device_id_type=MESH).start()

    for group, (first, last) in enumerate(RANK_GROUPS):
        count = last - jnp.maximum(rank, first - 1)

        @pl.when(is_chief & (count > 0))
        def _():
            pl.semaphore_wait(ready.at[group], count)
            signal(later_ok, data=other)
            for peer in FEAT_ORDER[first:last + 1]:
                pl.when(FEAT_RANK[peer] > rank)(lambda: send_block(peer, 1))

        @pl.when(jnp.logical_not(is_chief) & (count > 0))
        def _():
            pl.semaphore_wait(later_ok, 1)
            for peer in FEAT_ORDER[first:last + 1]:
                pl.when(FEAT_RANK[peer] > rank)(lambda: send_block(peer, 0))

    reg_row[...] = jnp.broadcast_to(reg_in[0], (1, 128))
    zero = jnp.float32(0)
    sources = [chief, chief - 1] + data_peers[1:]

    @pl.when(is_chief)
    def _():
        feat_tbl[...] = jnp.zeros_like(feat_tbl)
        thr_tbl[...] = jnp.zeros_like(thr_tbl)
        feat_tbl[0:7, 0:64] = feat_in[...]
        thr_tbl[0:7, 0:64] = thr_in[...]
        select, threshold = node_tables(feat_tbl[...], thr_tbl[...])
        for group in (1, 0):
            block = values.at[group]
            pltpu.make_async_copy(block, block, block_recv.at[group]).wait()
            s = chief - 1 + group
            table = values[group].reshape(NF * 8, CHUNK).astype(jnp.float32).astype(jnp.bfloat16)
            leaves[s] = route(table, select, threshold)
            for peer in DATA_ORDER:
                @pl.when(peer != d)
                def _():
                    pltpu.make_async_remote_copy(
                        src_ref=leaves.at[s], dst_ref=leaves.at[s], send_sem=leaf_send, recv_sem=leaf_recv.at[s],
                        device_id={'data': peer}, device_id_type=MESH).start()

    arrived = rows.at[pl.ds(0, ND - 1)]
    pltpu.make_async_copy(arrived, arrived, data_recv).wait()
    columns[...] = jnp.concatenate([rows[s, 0] for s in sources], axis=0).T

    def build(k):
        below[k] = jnp.where(columns[:, k:k + 1] <= iota((CHUNK, NBINS), 1).astype(jnp.float32), jnp.float32(1), zero).astype(jnp.bfloat16)

    def finish_sends():
        @pl.when(is_chief)
        def _():
            sent = values.at[0, pl.ds(0, NF - 1)]
            pltpu.make_async_copy(sent, sent, block_send).wait()
            told = leaves.at[pl.ds(0, ND - 1)]
            pltpu.make_async_copy(told, told, leaf_send).wait()
            pltpu.make_async_copy(told, told, leaf_send).wait()

        @pl.when(jnp.logical_not(is_chief))
        def _():
            sent = values.at[0]
            pltpu.make_async_copy(sent, sent, block_send).wait()
        pltpu.make_async_copy(arrived, arrived, data_send).wait()

    totals = [None, None]
    for k, s in enumerate(sources):
        for later in BUILD.get(k, ()):
            build(later)
        if k == ND - 1:
            finish_sends()
        arrival = pltpu.make_async_copy(leaves.at[s], leaves.at[s], leaf_recv.at[s])
        if k < 2:
            pl.when(jnp.logical_not(is_chief))(arrival.wait)
        else:
            arrival.wait()
        member = leaves[s] == iota((LEAVES, CHUNK), 0)
        mark = jnp.where(member, jnp.float32(1), zero).astype(jnp.bfloat16)
        for part in range(2):
            value = rows[s, 1 + part]
            inside = jnp.where(member, value, zero)
            leaf_sums[s, part] = inside[:, :128] + inside[:, 128:256] + (inside[:, 256:384] + inside[:, 384:])
            product = jnp.dot(jnp.concatenate([mark * piece for piece in split3(value)], axis=0), below[k], preferred_element_type=jnp.float32)
            product = product[:LEAVES] + product[LEAVES:2 * LEAVES] + product[2 * LEAVES:]
            totals[part] = product if k == 0 else totals[part] + product
    leaf_total = []
    for part in range(2):
        whole = leaf_sums[0, part]
        for s in range(1, ND):
            whole = whole + leaf_sums[s, part]
        leaf_total.append(jnp.sum(whole.T, axis=0, keepdims=True))
    leaf_row[...] = -leaf_total[0] / (leaf_total[1] + reg_row[...])
    for part in range(2):
        for half in range(2):
            sums[part, half] = totals[part][:, 128 * half:128 * (half + 1)]


def gain_kernel(*refs):
    pl.run_scoped(lambda out_sem: fill_gains(*refs, out_sem), pltpu.SemaphoreType.DMA((2,)))


def fill_gains(reg_row, sums, leaf_row, gain_hbm, leaf_hbm, heap, gains, out_sem):
    reg = reg_row[...]

    def score(g, h):
        return g * g / (h + reg)

    def fill(source, first, start, count):
        for r in range(start, start + count, 8):
            n = min(8, start + count - r)
            rows = pl.ds(r - first, n)
            all_g = source[0, 1, rows, 127:128]
            all_h = source[1, 1, rows, 127:128]
            whole = score(all_g, all_h)
            for half in range(2):
                left_g, left_h = source[0, half, rows, :], source[1, half, rows, :]
                gain = 0.5 * (score(left_g, left_h) + score(all_g - left_g, all_h - left_h) - whole)
                wide = 128 - half
                gains[pl.ds(r, n), 0, pl.ds(128 * half, wide)] = gain[:, :wide]
        pltpu.make_async_copy(gains.at[pl.ds(start, count)], gain_hbm.at[pl.ds(start, count)], out_sem.at[0]).start()

    leaf_copy = pltpu.make_async_copy(leaf_row, leaf_hbm, out_sem.at[1])
    leaf_copy.start()
    for level in range(6, -1, -1):
        n = 2 ** level
        source, base = (sums, 0) if level == 6 else (heap, 2 * n)
        for part in range(2):
            for half in range(2):
                heap[part, half, n:2 * n, :] = (source[part, half, pl.ds(base, n, stride=2), :]
                                                + source[part, half, pl.ds(base + 1, n, stride=2), :])
    fill(heap, -1, 0, 127)
    fill(sums, 127, 127, 64)
    fill(sums, 127, 191, 64)
    leaf_copy.wait()
    pltpu.make_async_copy(gains, gain_hbm, out_sem.at[0]).wait()


def solution(mesh):
    def per_device(binned, gradient, hessian, split_feat, split_thr, reg_lambda):
        hbm = pl.BlockSpec(memory_space=pltpu.HBM)
        vmem = pl.BlockSpec(memory_space=pltpu.VMEM)
        inputs = [binned.T, gradient.reshape(1, CHUNK), hessian.reshape(1, CHUNK), split_feat, split_thr]
        sums, leaf_row, reg_row = pl.pallas_call(
            exchange_kernel,
            out_shape=[
                jax.ShapeDtypeStruct((2, 2, LEAVES, 128), jnp.float32),
                jax.ShapeDtypeStruct((1, LEAVES), jnp.float32),
                jax.ShapeDtypeStruct((1, 128), jnp.float32),
            ],
            in_specs=[hbm] * 5 + [pl.BlockSpec(memory_space=pl.ANY)],
            out_specs=[vmem] * 3,
            scratch_shapes=[
                pltpu.VMEM((ND, 2, LEAVES, 128), jnp.float32),
                pltpu.VMEM((2, NF, 8, CHUNK), jnp.int32),
                pltpu.VMEM((ND, 3, 1, CHUNK), jnp.float32),
                pltpu.VMEM((ND, 3, 1, CHUNK), jnp.float32),
                pltpu.VMEM((CHUNK, ND), jnp.float32),
                pltpu.VMEM((ND, 1, CHUNK), jnp.int32),
                pltpu.VMEM((ND, CHUNK, NBINS), jnp.bfloat16),
                pltpu.VMEM((8, CHUNK), jnp.int32),
                pltpu.VMEM((1, CHUNK), jnp.float32),
                pltpu.VMEM((1, CHUNK), jnp.float32),
                pltpu.SMEM((1,), jnp.float32),
                pltpu.VMEM((7, 64), jnp.int32),
                pltpu.VMEM((7, 64), jnp.int32),
                pltpu.VMEM((8, 128), jnp.int32),
                pltpu.VMEM((8, 128), jnp.int32),
            ],
            compiler_params=pltpu.CompilerParams(collective_id=0, has_side_effects=True, vmem_limit_bytes=24 * 2 ** 20),
            name='exchange',
        )(*[pltpu.with_memory_space_constraint(a, pltpu.HBM) for a in inputs], reg_lambda)
        gain, leaf_value = pl.pallas_call(
            gain_kernel,
            out_shape=[
                jax.ShapeDtypeStruct((255, 1, 255), jnp.float32),
                jax.ShapeDtypeStruct((1, LEAVES), jnp.float32),
            ],
            in_specs=[vmem] * 3,
            out_specs=[hbm] * 2,
            scratch_shapes=[
                pltpu.VMEM((2, 2, LEAVES, 128), jnp.float32),
                pltpu.VMEM((255, 1, 255), jnp.float32),
            ],
            compiler_params=pltpu.CompilerParams(vmem_limit_bytes=24 * 2 ** 20),
            name='gains',
        )(reg_row, sums, leaf_row)
        return gain, leaf_value.reshape(LEAVES)

    row_spec = P(('tree', 'data'))
    return jax.shard_map(
        per_device,
        mesh=mesh,
        in_specs=(P(('tree', 'data'), 'feat'), row_spec, row_spec, P('tree', None), P('tree', None), P(None)),
        out_specs=(P('tree', ('feat', 'data'), None), P('tree')),
        check_vma=False,
    )
```

```python
import jax
import jax.numpy as jnp
from jax import lax
from jax.experimental import pallas as pl
from jax.experimental.pallas import tpu as pltpu
from jax.sharding import PartitionSpec as P

NBINS = 256
SIDE = 4
NF = SIDE * SIDE
ND = 8
CHUNK = 512
LEAVES = 128
HUB = 0
LATER_ORDER = (4, 3, 8, 7, 1, 12, 5, 0, 6, 10, 9, 11, 13, 15, 2, 14)
FEAT_ORDER = (0, 1, 2, 4, 3, 8, 7, 5, 12, 6, 10, 9, 11, 14, 13, 15)
FEAT_RANK = [FEAT_ORDER.index(f) for f in range(NF)]
BUILD = {0: (0,), 1: (1,), 2: (2, 3), 3: (4, 5, 6, 7)}
SEND_ORDER = (0, 8, 3, 9, 4, 1, 11, 7, 12, 13, 5, 6, 14, 10, 2, 15)
RANK_GROUPS = ((0, 7), (8, 15))
DATA_ORDER = (1, 0, 3, 2, 5, 4, 7, 6)
MESH = pl.DeviceIdType.MESH


def split3(value):
    largest = float(jnp.finfo(jnp.bfloat16).max)
    first = jnp.clip(value, -largest, largest).astype(jnp.bfloat16)
    rest = value - first.astype(jnp.float32)
    second = rest.astype(jnp.bfloat16)
    third = (rest - second.astype(jnp.float32)).astype(jnp.bfloat16)
    return first, second, third


def iota(shape, dim):
    return lax.broadcasted_iota(jnp.int32, shape, dim)


def contract_lanes(left, right):
    return lax.dot_general(left, right, (((1,), (1,)), ((), ())), preferred_element_type=jnp.float32)


def node_tables(feat_tbl, thr_tbl):
    lane = iota((8, 128), 1)
    feat_row = jnp.zeros((1, 128), jnp.int32)
    thr_row = jnp.zeros((1, 128), jnp.int32)
    for level in range(7):
        here = (lane >= 2 ** level) & (lane < 2 ** (level + 1))
        feat_row = feat_row + jnp.where(here, pltpu.roll(feat_tbl, 2 ** level, 1), 0)[level:level + 1]
        thr_row = thr_row + jnp.where(here, pltpu.roll(thr_tbl, 2 ** level, 1), 0)[level:level + 1]
    one, zero = jnp.float32(1), jnp.float32(0)
    by_feat = jnp.where(feat_row == iota((128, 128), 0), one, zero).astype(jnp.bfloat16)
    by_thr = jnp.broadcast_to(thr_row.astype(jnp.float32), (128, 128)).astype(jnp.bfloat16)
    position = iota((128, 128), 0)
    reverse = jnp.zeros((128, 128), jnp.int32)
    for bit in range(7):
        reverse = reverse | (((position >> bit) & 1) << (6 - bit))
    heap = jnp.zeros((128, 128), jnp.int32)
    for level in range(7):
        heap = jnp.where(position >= 2 ** level, 2 ** level + (reverse >> (7 - level)), heap)
    order = jnp.where(heap == iota((128, 128), 1), one, zero).astype(jnp.bfloat16)
    return contract_lanes(order, by_feat).astype(jnp.bfloat16), contract_lanes(order, by_thr)


def route(values, select, threshold):
    picked = jnp.dot(select, values, preferred_element_type=jnp.float32)
    limit = jnp.concatenate([threshold] * (values.shape[1] // 128), axis=1)
    right = picked > limit
    leaf = jnp.where(right[64:128], 1, 0)
    for level in range(5, -1, -1):
        n = 2 ** level
        leaf = jnp.where(right[n:2 * n], leaf[n:] + 2 ** (6 - level), leaf[:n])
    return leaf


def exchange_kernel(*refs):
    dma, regular = pltpu.SemaphoreType.DMA, pltpu.SemaphoreType.REGULAR
    pl.run_scoped(
        lambda *own: exchange(*refs, *own),
        regular((len(RANK_GROUPS),)), regular, regular, regular, regular,
        dma((2,)), dma, dma((ND,)), dma((6,)), dma, dma, dma)


def exchange(bin_hbm, grad_hbm, hess_hbm, feat_hbm, thr_hbm, reg_hbm, sums, leaf_row, reg_row,
                    leaf_sums, values, parcels, rows, columns, leaves, below, own_bins, own_grad, own_hess, reg_in, feat_in, thr_in, feat_tbl, thr_tbl,
                    ready, gathered, everyone, earlier_ok, later_ok, block_recv, data_recv, leaf_recv,
                    local_sem, block_send, data_send, leaf_send):
    f, d = lax.axis_index('feat'), lax.axis_index('data')
    x, core = d // 2, d % 2
    chief, other = 2 * x + 1, 2 * x + 1 - core
    near = x + 1 - 2 * (x % 2)
    lines = [near, (x + 2) % SIDE, SIDE - 1 - x]
    data_peers = [other] + [2 * line + c for c in (1, 0) for line in lines]
    rank = sum(jnp.where(f == peer, FEAT_RANK[peer], 0) for peer in range(NF))
    is_chief = core == 1

    own = pltpu.make_async_copy(bin_hbm, values.at[1, f], block_recv.at[1])
    local = [
        pltpu.make_async_copy(bin_hbm, own_bins, local_sem.at[0]),
        pltpu.make_async_copy(grad_hbm, own_grad, local_sem.at[1]),
        pltpu.make_async_copy(hess_hbm, own_hess, local_sem.at[2]),
        pltpu.make_async_copy(feat_hbm, feat_in, local_sem.at[3]),
        pltpu.make_async_copy(thr_hbm, thr_in, local_sem.at[4]),
        pltpu.make_async_copy(reg_hbm, reg_in, local_sem.at[5]),
    ]
    barrier = pltpu.get_barrier_semaphore()

    def signal(semaphore, **device):
        pl.semaphore_signal(semaphore, inc=1, device_id=device, device_id_type=MESH)

    def send_block(peer, group):
        pltpu.make_async_remote_copy(
            src_ref=bin_hbm, dst_ref=values.at[group, f], send_sem=block_send, recv_sem=block_recv.at[group],
            device_id={'feat': peer, 'data': chief}, device_id_type=MESH).start()

    @pl.when(is_chief)
    def _():
        for peer in reversed(FEAT_ORDER):
            pl.when(FEAT_RANK[peer] > rank)(lambda: signal(barrier, feat=peer))
        signal(barrier, data=other)
        own.start()

    @pl.when(jnp.logical_not(is_chief))
    def _():
        signal(barrier, data=other)

        @pl.when(d == HUB)
        def _():
            for peer in range(2, ND, 2):
                signal(barrier, data=peer)
    for copy in local:
        copy.start()

    @pl.when(is_chief)
    def _():
        pl.semaphore_wait(barrier, rank + 1)
        signal(earlier_ok, data=other)
        for peer in SEND_ORDER:
            pl.when(FEAT_RANK[peer] < rank)(lambda: send_block(peer, 1))
        own_group = sum(jnp.where(rank >= first, 1, 0) for first, _ in RANK_GROUPS) - 1
        for peer in FEAT_ORDER:
            pl.when(FEAT_RANK[peer] < rank)(lambda: signal(ready.at[own_group], feat=peer))

    @pl.when(jnp.logical_not(is_chief))
    def _():
        pl.semaphore_wait(barrier, jnp.where(d == HUB, 1, 2))
        pl.when(d != HUB)(lambda: signal(gathered, data=HUB))
        pl.semaphore_wait(earlier_ok, 1)
        for peer in SEND_ORDER:
            pl.when(FEAT_RANK[peer] <= rank)(lambda: send_block(peer, 0))

    for copy in local:
        copy.wait()
    for peer in range(ND):
        parcels[peer, 0] = own_bins[peer:peer + 1, :].astype(jnp.float32)
        parcels[peer, 1] = own_grad[...]
        parcels[peer, 2] = own_hess[...]
    rows[d] = parcels[d]

    @pl.when(d == HUB)
    def _():
        pl.semaphore_wait(gathered, SIDE - 1)
        for peer in data_peers:
            signal(everyone, data=peer)

    @pl.when(d != HUB)
    def _():
        pl.semaphore_wait(everyone, 1)
    for peer in data_peers:
        pltpu.make_async_remote_copy(
            src_ref=parcels.at[peer], dst_ref=rows.at[d], send_sem=data_send, recv_sem=data_recv,
            device_id={'data': peer}, device_id_type=MESH).start()

    for group, (first, last) in enumerate(RANK_GROUPS):
        count = last - jnp.maximum(rank, first - 1)

        @pl.when(is_chief & (count > 0))
        def _():
            pl.semaphore_wait(ready.at[group], count)
            signal(later_ok, data=other)
            for peer in [p for p in LATER_ORDER if first <= FEAT_RANK[p] <= last]:
                pl.when(FEAT_RANK[peer] > rank)(lambda: send_block(peer, 1))

        @pl.when(jnp.logical_not(is_chief) & (count > 0))
        def _():
            pl.semaphore_wait(later_ok, 1)
            for peer in [p for p in LATER_ORDER if first <= FEAT_RANK[p] <= last]:
                pl.when(FEAT_RANK[peer] > rank)(lambda: send_block(peer, 0))

    reg_row[...] = jnp.broadcast_to(reg_in[0], (1, 128))
    zero = jnp.float32(0)
    sources = [chief, chief - 1] + data_peers[1:]

    @pl.when(is_chief)
    def _():
        feat_tbl[...] = jnp.zeros_like(feat_tbl)
        thr_tbl[...] = jnp.zeros_like(thr_tbl)
        feat_tbl[0:7, 0:64] = feat_in[...]
        thr_tbl[0:7, 0:64] = thr_in[...]
        select, threshold = node_tables(feat_tbl[...], thr_tbl[...])
        for group in (1, 0):
            block = values.at[group]
            pltpu.make_async_copy(block, block, block_recv.at[group]).wait()
            s = chief - 1 + group
            table = values[group].reshape(NF * 8, CHUNK).astype(jnp.float32).astype(jnp.bfloat16)
            leaves[s] = route(table, select, threshold)
            for peer in DATA_ORDER:
                @pl.when(peer != d)
                def _():
                    pltpu.make_async_remote_copy(
                        src_ref=leaves.at[s], dst_ref=leaves.at[s], send_sem=leaf_send, recv_sem=leaf_recv.at[s],
                        device_id={'data': peer}, device_id_type=MESH).start()

    arrived = rows.at[pl.ds(0, ND - 1)]
    pltpu.make_async_copy(arrived, arrived, data_recv).wait()
    columns[...] = jnp.concatenate([rows[s, 0] for s in sources], axis=0).T

    def build(k):
        below[k] = jnp.where(columns[:, k:k + 1] <= iota((CHUNK, NBINS), 1).astype(jnp.float32), jnp.float32(1), zero).astype(jnp.bfloat16)

    def finish_sends():
        @pl.when(is_chief)
        def _():
            sent = values.at[0, pl.ds(0, NF - 1)]
            pltpu.make_async_copy(sent, sent, block_send).wait()
            told = leaves.at[pl.ds(0, ND - 1)]
            pltpu.make_async_copy(told, told, leaf_send).wait()
            pltpu.make_async_copy(told, told, leaf_send).wait()

        @pl.when(jnp.logical_not(is_chief))
        def _():
            sent = values.at[0]
            pltpu.make_async_copy(sent, sent, block_send).wait()
        pltpu.make_async_copy(arrived, arrived, data_send).wait()

    totals = [None, None]
    for k, s in enumerate(sources):
        for later in BUILD.get(k, ()):
            build(later)
        if k == ND - 1:
            finish_sends()
        arrival = pltpu.make_async_copy(leaves.at[s], leaves.at[s], leaf_recv.at[s])
        if k < 2:
            pl.when(jnp.logical_not(is_chief))(arrival.wait)
        else:
            arrival.wait()
        member = leaves[s] == iota((LEAVES, CHUNK), 0)
        mark = jnp.where(member, jnp.float32(1), zero).astype(jnp.bfloat16)
        for part in range(2):
            value = rows[s, 1 + part]
            inside = jnp.where(member, value, zero)
            leaf_sums[s, part] = inside[:, :128] + inside[:, 128:256] + (inside[:, 256:384] + inside[:, 384:])
            product = jnp.dot(jnp.concatenate([mark * piece for piece in split3(value)], axis=0), below[k], preferred_element_type=jnp.float32)
            product = product[:LEAVES] + product[LEAVES:2 * LEAVES] + product[2 * LEAVES:]
            totals[part] = product if k == 0 else totals[part] + product
    leaf_total = []
    for part in range(2):
        whole = leaf_sums[0, part]
        for s in range(1, ND):
            whole = whole + leaf_sums[s, part]
        leaf_total.append(jnp.sum(whole.T, axis=0, keepdims=True))
    leaf_row[...] = -leaf_total[0] / (leaf_total[1] + reg_row[...])
    for part in range(2):
        for half in range(2):
            sums[part, half] = totals[part][:, 128 * half:128 * (half + 1)]


def gain_kernel(*refs):
    pl.run_scoped(lambda out_sem: fill_gains(*refs, out_sem), pltpu.SemaphoreType.DMA((2,)))


def fill_gains(reg_row, sums, leaf_row, gain_hbm, leaf_hbm, heap, gains, out_sem):
    reg = reg_row[...]

    def score(g, h):
        return g * g / (h + reg)

    def fill(source, first, start, count):
        for r in range(start, start + count, 8):
            n = min(8, start + count - r)
            rows = pl.ds(r - first, n)
            all_g = source[0, 1, rows, 127:128]
            all_h = source[1, 1, rows, 127:128]
            whole = score(all_g, all_h)
            for half in range(2):
                left_g, left_h = source[0, half, rows, :], source[1, half, rows, :]
                gain = 0.5 * (score(left_g, left_h) + score(all_g - left_g, all_h - left_h) - whole)
                wide = 128 - half
                gains[pl.ds(r, n), 0, pl.ds(128 * half, wide)] = gain[:, :wide]
        pltpu.make_async_copy(gains.at[pl.ds(start, count)], gain_hbm.at[pl.ds(start, count)], out_sem.at[0]).start()

    leaf_copy = pltpu.make_async_copy(leaf_row, leaf_hbm, out_sem.at[1])
    leaf_copy.start()
    for level in range(6, -1, -1):
        n = 2 ** level
        source, base = (sums, 0) if level == 6 else (heap, 2 * n)
        for part in range(2):
            for half in range(2):
                heap[part, half, n:2 * n, :] = (source[part, half, pl.ds(base, n, stride=2), :]
                                                + source[part, half, pl.ds(base + 1, n, stride=2), :])
    fill(heap, -1, 0, 127)
    fill(sums, 127, 127, 64)
    fill(sums, 127, 191, 64)
    leaf_copy.wait()
    pltpu.make_async_copy(gains, gain_hbm, out_sem.at[0]).wait()


def solution(mesh):
    def per_device(binned, gradient, hessian, split_feat, split_thr, reg_lambda):
        hbm = pl.BlockSpec(memory_space=pltpu.HBM)
        vmem = pl.BlockSpec(memory_space=pltpu.VMEM)
        inputs = [binned.T, gradient.reshape(1, CHUNK), hessian.reshape(1, CHUNK), split_feat, split_thr]
        sums, leaf_row, reg_row = pl.pallas_call(
            exchange_kernel,
            out_shape=[
                jax.ShapeDtypeStruct((2, 2, LEAVES, 128), jnp.float32),
                jax.ShapeDtypeStruct((1, LEAVES), jnp.float32),
                jax.ShapeDtypeStruct((1, 128), jnp.float32),
            ],
            in_specs=[hbm] * 5 + [pl.BlockSpec(memory_space=pl.ANY)],
            out_specs=[vmem] * 3,
            scratch_shapes=[
                pltpu.VMEM((ND, 2, LEAVES, 128), jnp.float32),
                pltpu.VMEM((2, NF, 8, CHUNK), jnp.int32),
                pltpu.VMEM((ND, 3, 1, CHUNK), jnp.float32),
                pltpu.VMEM((ND, 3, 1, CHUNK), jnp.float32),
                pltpu.VMEM((CHUNK, ND), jnp.float32),
                pltpu.VMEM((ND, 1, CHUNK), jnp.int32),
                pltpu.VMEM((ND, CHUNK, NBINS), jnp.bfloat16),
                pltpu.VMEM((8, CHUNK), jnp.int32),
                pltpu.VMEM((1, CHUNK), jnp.float32),
                pltpu.VMEM((1, CHUNK), jnp.float32),
                pltpu.SMEM((1,), jnp.float32),
                pltpu.VMEM((7, 64), jnp.int32),
                pltpu.VMEM((7, 64), jnp.int32),
                pltpu.VMEM((8, 128), jnp.int32),
                pltpu.VMEM((8, 128), jnp.int32),
            ],
            compiler_params=pltpu.CompilerParams(collective_id=0, has_side_effects=True, vmem_limit_bytes=24 * 2 ** 20),
            name='exchange',
        )(*[pltpu.with_memory_space_constraint(a, pltpu.HBM) for a in inputs], reg_lambda)
        gain, leaf_value = pl.pallas_call(
            gain_kernel,
            out_shape=[
                jax.ShapeDtypeStruct((255, 1, 255), jnp.float32),
                jax.ShapeDtypeStruct((1, LEAVES), jnp.float32),
            ],
            in_specs=[vmem] * 3,
            out_specs=[hbm] * 2,
            scratch_shapes=[
                pltpu.VMEM((2, 2, LEAVES, 128), jnp.float32),
                pltpu.VMEM((255, 1, 255), jnp.float32),
            ],
            compiler_params=pltpu.CompilerParams(vmem_limit_bytes=24 * 2 ** 20),
            name='gains',
        )(reg_row, sums, leaf_row)
        return gain, leaf_value.reshape(LEAVES)

    row_spec = P(('tree', 'data'))
    return jax.shard_map(
        per_device,
        mesh=mesh,
        in_specs=(P(('tree', 'data'), 'feat'), row_spec, row_spec, P('tree', None), P('tree', None), P(None)),
        out_specs=(P('tree', ('feat', 'data'), None), P('tree')),
        check_vma=False,
    )
```
